128 devices in a mesh: dp: 1, ep: 128 (over z, y, x, core).
Axes of the slice: x: 4, y: 4, z: 4, core: 2. Of those that a mesh axis runs over, the one named last changes fastest.
Arguments:
- x_a: bfloat16 [4096, 2048], P(('dp', 'ep'))
- route_a: int32 [4096, 8], P(('dp', 'ep'))
- gate_a: float32 [4096, 8], P(('dp', 'ep'))
- h_b: bfloat16 [4096, 2048], P(('dp', 'ep'))
- attn_b: bfloat16 [4096, 4096], P(('dp', 'ep'))
- route_b: int32 [4096, 8], P(('dp', 'ep'))
- gate_b: float32 [4096, 8], P(('dp', 'ep'))
- w_qkv: bfloat16 [2048, 5120], replicated
- w_o: bfloat16 [4096, 2048], replicated
- w_gate: bfloat16 [128, 2048, 768], P('ep')
- w_up: bfloat16 [128, 2048, 768], P('ep')
- w_down: bfloat16 [128, 768, 2048], P('ep')
Outputs:
- output 1: bfloat16 [4096, 2048], P(('dp', 'ep'))
- output 2: bfloat16 [4096, 2048], P(('dp', 'ep'))
- output 3: bfloat16 [4096, 5120], P(('dp', 'ep'))
All inputs are finite; a program needn't handle non-finite values.
Results may differ from the reference program's by a relative error of at most 0.0107943.
Values are sent between devices in bfloat16 or wider.
A program may use at most 1 GiB of HBM per device.

```python
import jax
import jax.numpy as jnp
from jax import lax

MODEL_DIM = 2048
FF_DIM = 768
NUM_EXPERTS = 128
TOP_K = 8
NUM_HEADS = 32
KV_HEADS = 4
HEAD_DIM = 128
TOKENS_DEV = 32
GROUP_DEVS = 128

CAPACITY = min(TOKENS_DEV, 2 * ((TOKENS_DEV * TOP_K + NUM_EXPERTS - 1) // NUM_EXPERTS))
LOCAL_EXPERTS = NUM_EXPERTS // GROUP_DEVS
QKV_DIM = (NUM_HEADS + 2 * KV_HEADS) * HEAD_DIM
ATTN_DIM = NUM_HEADS * HEAD_DIM
GROUP_ROWS = GROUP_DEVS * TOKENS_DEV
HOT_DEVS = max(1, GROUP_DEVS // 4)


def source_routing(rng_key, dev_order):
    key_local, key_want, key_rows = jax.random.split(rng_key, 3)
    local_order = jax.vmap(lambda sub_key: jax.random.permutation(sub_key, LOCAL_EXPERTS))(jax.random.split(key_local, GROUP_DEVS))
    visits = jnp.arange(NUM_EXPERTS)
    visit_dev = dev_order[visits % GROUP_DEVS]
    visit_expert = visit_dev * LOCAL_EXPERTS + local_order[visit_dev, visits // GROUP_DEVS]
    wanted = jax.random.randint(key_want, (NUM_EXPERTS,), 1, CAPACITY + 1)
    wanted = jnp.where(visits % GROUP_DEVS < HOT_DEVS, CAPACITY, wanted)
    wanted = jnp.where(visits < GROUP_DEVS, 1, wanted)
    wanted = jnp.where(visits == 0, CAPACITY, wanted)
    n_entries = TOKENS_DEV * TOP_K
    first_pass = jnp.clip(n_entries - (jnp.cumsum(wanted) - wanted), 0, wanted)
    room_left = CAPACITY - first_pass
    left_over = n_entries - jnp.sum(first_pass)
    second_pass = jnp.clip(left_over - (jnp.cumsum(room_left) - room_left), 0, room_left)
    run_ends = jnp.cumsum(first_pass + second_pass)
    positions = jnp.arange(n_entries)
    run_index = jnp.sum((run_ends[None, :] <= positions[:, None]).astype(jnp.int32), axis=1)
    choices = visit_expert[run_index].reshape(TOP_K, TOKENS_DEV).T
    return choices[jax.random.permutation(key_rows, TOKENS_DEV)]


def group_routing(rng_key):
    key_order, key_src = jax.random.split(rng_key)
    dev_order = jax.random.permutation(key_order, GROUP_DEVS)
    per_source = jax.vmap(lambda sub_key: source_routing(sub_key, dev_order))(jax.random.split(key_src, GROUP_DEVS))
    return per_source.reshape(GROUP_ROWS, TOP_K).astype(jnp.int32)


def setup_inputs(seed: int = 0, part: int = 0) -> dict:
    root_key = jax.random.key(seed)
    shared_keys = jax.random.split(jax.random.fold_in(root_key, 1), 5)
    part_keys = jax.random.split(jax.random.fold_in(jax.random.fold_in(root_key, 2), part), 7)

    def normal_bf16(sub_key, arr_shape, scale_by):
        return (jax.random.normal(sub_key, arr_shape, jnp.float32) * scale_by).astype(jnp.bfloat16)

    return {
        'x_a': normal_bf16(part_keys[0], (GROUP_ROWS, MODEL_DIM), 1.0),
        'route_a': group_routing(part_keys[1]),
        'gate_a': jax.nn.softmax(jax.random.normal(part_keys[2], (GROUP_ROWS, TOP_K), jnp.float32), axis=-1),
        'h_b': normal_bf16(part_keys[3], (GROUP_ROWS, MODEL_DIM), 1.0),
        'attn_b': normal_bf16(part_keys[4], (GROUP_ROWS, ATTN_DIM), 1.0),
        'route_b': group_routing(part_keys[5]),
        'gate_b': jax.nn.softmax(jax.random.normal(part_keys[6], (GROUP_ROWS, TOP_K), jnp.float32), axis=-1),
        'w_qkv': normal_bf16(shared_keys[0], (MODEL_DIM, QKV_DIM), MODEL_DIM ** -0.5),
        'w_o': normal_bf16(shared_keys[1], (ATTN_DIM, MODEL_DIM), ATTN_DIM ** -0.5),
        'w_gate': normal_bf16(shared_keys[2], (NUM_EXPERTS, MODEL_DIM, FF_DIM), MODEL_DIM ** -0.5),
        'w_up': normal_bf16(shared_keys[3], (NUM_EXPERTS, MODEL_DIM, FF_DIM), MODEL_DIM ** -0.5),
        'w_down': normal_bf16(shared_keys[4], (NUM_EXPERTS, FF_DIM, MODEL_DIM), FF_DIM ** -0.5),
    }


def expert_layer(tokens, route_ids, gate_vals, w_gate, w_up, w_down):
    n_entries = GROUP_ROWS * TOP_K
    per_source = route_ids.reshape(GROUP_DEVS, TOKENS_DEV * TOP_K)
    one_hot = (per_source[:, :, None] == jnp.arange(NUM_EXPERTS)[None, None, :]).astype(jnp.int32)
    slot_rank = jnp.sum((jnp.cumsum(one_hot, axis=1) - 1) * one_hot, axis=2)
    buffer_row = jnp.arange(GROUP_DEVS)[:, None] * CAPACITY + slot_rank
    entry_ids = jnp.arange(n_entries)
    slot_table = jnp.full((NUM_EXPERTS, GROUP_DEVS * CAPACITY), n_entries, jnp.int32)
    slot_table = slot_table.at[per_source.reshape(-1), buffer_row.reshape(-1)].set(entry_ids)
    padded = jnp.concatenate([tokens, jnp.zeros((1, MODEL_DIM), tokens.dtype)], axis=0)

    def one_expert(results, inputs):
        rows_ids, gate_w, up_w, down_w = inputs
        expert_in = padded[rows_ids // TOP_K]
        gate_act = jnp.dot(expert_in, gate_w, preferred_element_type=jnp.float32)
        up_act = jnp.dot(expert_in, up_w, preferred_element_type=jnp.float32)
        hidden = (jax.nn.silu(gate_act) * up_act).astype(jnp.bfloat16)
        expert_out = jnp.dot(hidden, down_w, preferred_element_type=jnp.float32).astype(jnp.bfloat16)
        return results.at[rows_ids].set(expert_out), None

    results = jnp.zeros((n_entries + 1, MODEL_DIM), jnp.bfloat16)
    results = lax.scan(one_expert, results, (slot_table, w_gate, w_up, w_down))[0]
    per_choice = results[:n_entries].reshape(GROUP_ROWS, TOP_K, MODEL_DIM)
    mixture = jnp.zeros((GROUP_ROWS, MODEL_DIM), jnp.float32)
    for choice in range(TOP_K):
        mixture = mixture + gate_vals[:, choice:choice + 1] * per_choice[:, choice].astype(jnp.float32)
    return (tokens.astype(jnp.float32) + mixture).astype(jnp.bfloat16)


def reference(x_a, route_a, gate_a, h_b, attn_b, route_b, gate_b, w_qkv, w_o, w_gate, w_up, w_down):
    out_a = expert_layer(x_a, route_a, gate_a, w_gate, w_up, w_down)
    qkv_b = jnp.dot(h_b, w_qkv, preferred_element_type=jnp.float32).astype(jnp.bfloat16)
    proj_b = jnp.dot(attn_b, w_o, preferred_element_type=jnp.float32).astype(jnp.bfloat16)
    mid_b = (h_b.astype(jnp.float32) + proj_b.astype(jnp.float32)).astype(jnp.bfloat16)
    out_b = expert_layer(mid_b, route_b, gate_b, w_gate, w_up, w_down)
    return (out_a, out_b, qkv_b)
```

```python
import functools

import jax
import jax.numpy as jnp
from jax import lax
from jax.experimental import pallas as pl
from jax.experimental.pallas import tpu as pltpu
from jax.sharding import PartitionSpec as P

MESH = pl.DeviceIdType.MESH
BF16 = jnp.bfloat16
F32 = jnp.float32

SIDE = 4
CORES = 2
TOK = 32
CAP = 4
TOP_K = 8
D = 2048
N_EXP = 128
FF = 768
ATT = 4096
QKV = 5120
SLOTS = N_EXP * CAP
CLASSES = ((0, 1, 2), (1, 2, 0), (2, 0, 1))
WIDTHS = (768, 640, 640)
STARTS = (0, 768, 1408)
STRIDE = (32, 8, 2)
UNUSED = 8.0
WO_CHUNK = 512
WQ_CHUNK = 256


def iota(shape, dim):
    return lax.broadcasted_iota(jnp.int32, shape, dim)


def dot(a, b):
    return jnp.dot(a, b, preferred_element_type=F32)


def dot_nt(a, b):
    return lax.dot_general(a, b, (((1,), (1,)), ((), ())), preferred_element_type=F32)


def slot_fields(cls, idx):
    d1, d2, d3 = CLASSES[cls]
    out = {d3: idx >> 7, d2: (idx >> 4) & 3, d1: (idx >> 2) & 3}
    return out, (idx >> 6) & 1, idx & 3


def slot_index(cls, coords, core, rank):
    d1, d2, d3 = CLASSES[cls]
    return (coords[d3] << 7) | (core << 6) | (coords[d2] << 4) | (coords[d1] << 2) | rank


def reorder(to_cls, from_cls):
    row = iota((SLOTS, 1), 0)
    coords, core, rank = slot_fields(to_cls, row)
    want = slot_index(from_cls, coords, core, rank)
    return (iota((SLOTS, SLOTS), 1) == want).astype(F32).astype(BF16)


class Links:
    def __init__(self, send, recv):
        self.send, self.recv, self.used, self.open = send, recv, 0, []

    def copy(self, src, dst, device):
        i = self.used
        self.used += 1
        op = pltpu.make_async_remote_copy(
            src_ref=src, dst_ref=dst, send_sem=self.send.at[i], recv_sem=self.recv.at[i],
            device_id={"ep": device}, device_id_type=MESH)
        op.start()
        self.open.append(op)
        return op

    def drain(self):
        for op in self.open:
            op.wait_send()


def n_copies():
    return 2 * (9 + 9 + 9 + 21 + 21 + 9 + 9)


def kernel(*refs):
    it = iter(refs)
    take = lambda n: [next(it) for _ in range(n)]
    x_a, h_b, attn, route_a, route_b, gate_a, gate_b = take(7)
    w_qkv, w_o, w_gate, w_up, w_down = take(5)
    out_a, out_b, qkv_out = take(3)
    bufs = []
    for _ in range(2):
        b = {}
        for name in ("ag", "ps", "pr", "r1", "r2", "sm", "r3", "gg"):
            b[name] = take(3)
        bufs.append(b)
    xbuf, hbuf, perms, proj_acc, qkv_acc, u_b = take(6)
    vg, vu, vd, wo_buf, wq_buf = take(5)
    send_sem, recv_sem, w_sem, wo_sem, wq_sem = take(5)

    me = lax.axis_index("ep")
    core = lax.rem(me, 2)
    pos = [lax.rem(me // 32, 4), lax.rem(me // 8, 4), lax.rem(me // 2, 4)]
    links = Links(send_sem, recv_sem)

    def along(dim, off):
        there = lax.rem(pos[dim] + off, 4)
        return there, me + (there - pos[dim]) * STRIDE[dim]

    peers = []
    for dim in range(3):
        for off in (1, 2, 3):
            _, dev = along(dim, off)
            peers += [dev, dev + 1 - 2 * core]
    peers.append(me + 1 - 2 * core)
    barrier = pltpu.get_barrier_semaphore()
    for dev in peers:
        pl.semaphore_signal(barrier, inc=1, device_id={"ep": dev}, device_id_type=MESH)

    w_copies = [pltpu.make_async_copy(src.at[0], dst, w_sem.at[i])
                for i, (src, dst) in enumerate(((w_gate, vg), (w_up, vu), (w_down, vd)))]
    n_wo, n_wq = ATT // WO_CHUNK, D // WQ_CHUNK

    def wo_copy(i):
        return pltpu.make_async_copy(w_o.at[pl.ds(i * WO_CHUNK, WO_CHUNK)], wo_buf.at[i % 2], wo_sem.at[i % 2])

    def wq_copy(i):
        return pltpu.make_async_copy(w_qkv.at[pl.ds(i * WQ_CHUNK, WQ_CHUNK)], wq_buf.at[i % 2], wq_sem.at[i % 2])

    wo_copy(0).start()
    wo_copy(1).start()
    for c in w_copies:
        c.start()
    wq_copy(0).start()
    wq_copy(1).start()

    def proj_step(i):
        wo_copy(i).wait()
        part = dot(attn[:, i * WO_CHUNK:(i + 1) * WO_CHUNK], wo_buf[i % 2])
        proj_acc[...] = part if i == 0 else proj_acc[...] + part
        if i + 2 < n_wo:
            wo_copy(i + 2).start()

    def qkv_step(i):
        wq_copy(i).wait()
        part = dot(h_b[:, i * WQ_CHUNK:(i + 1) * WQ_CHUNK], wq_buf[i % 2])
        if i == n_wq - 1:
            qkv_out[...] = (qkv_acc[...] + part).astype(BF16)
        else:
            qkv_acc[...] = part if i == 0 else qkv_acc[...] + part
        if i + 2 < n_wq:
            wq_copy(i + 2).start()

    def prepare(b, rows, route, gate):
        lane = iota((TOK, N_EXP), 1)
        chosen = jnp.zeros((TOK, N_EXP), F32)
        gates = jnp.zeros((TOK, N_EXP), F32)
        for j in range(TOP_K):
            hit = route[:, j:j + 1] == lane
            chosen = jnp.where(hit, 1.0, chosen)
            gates = jnp.where(hit, gate[:, j:j + 1], gates)
        before = (iota((TOK, TOK), 0) > iota((TOK, TOK), 1)).astype(F32).astype(BF16)
        rank = dot(before, chosen.astype(BF16))
        rank = jnp.where(chosen > 0.5, rank, UNUSED).astype(BF16)
        for cls, (d1, d2, d3) in enumerate(CLASSES):
            w, s = WIDTHS[cls], STARTS[cls]
            b["ag"][cls][pos[d2], pos[d1], :, :w] = rows[:, s:s + w]
            b["ag"][cls][pos[d2], pos[d1], :, w:] = rank
            b["gg"][cls][pos[d1]] = gates

    def gather1(b):
        ops = []
        for cls, (d1, d2, d3) in enumerate(CLASSES):
            mine = b["ag"][cls].at[pos[d2], pos[d1]]
            for off in (2, 1, 3):
                ops.append(links.copy(mine, mine, along(d1, off)[1]))
        return ops

    def gather_gates(b):
        ops = []
        for cls, (d1, d2, d3) in enumerate(CLASSES):
            mine = b["gg"][cls].at[pos[d1]]
            for off in (2, 1, 3):
                ops.append(links.copy(mine, mine, along(d1, off)[1]))
        return ops

    def gather2(b, ops1):
        ops = []
        for cls, (d1, d2, d3) in enumerate(CLASSES):
            for op in ops1[3 * cls:3 * cls + 3]:
                op.wait_recv()
            mine = b["ag"][cls].at[pos[d2]]
            for off in (2, 1, 3):
                ops.append(links.copy(mine, mine, along(d2, off)[1]))
        return ops

    def exchange(b, ops2):
        ops = []
        n = CORES * 64
        slot = iota((n, 1), 0)
        src_mask = ((slot >> 2) & 15) == (iota((n, SIDE * SIDE * TOK), 1) >> 5)
        kth = (slot & 3).astype(F32)
        for cls, (d1, d2, d3) in enumerate(CLASSES):
            w = WIDTHS[cls]
            for op in ops2[3 * cls:3 * cls + 3]:
                op.wait_recv()
            ag, ps, pr = b["ag"][cls], b["ps"][cls], b["pr"][cls]
            ranks = ag[:, :, :, w:].reshape(SIDE * SIDE * TOK, N_EXP)
            for off in (2, 1, 3, 0):
                there, dev = along(d3, off)
                first = dev - core
                pick_exp = (iota((n, N_EXP), 1) == first + (slot >> 6)).astype(F32).astype(BF16)
                val = dot_nt(pick_exp, ranks)
                pick = jnp.where(src_mask & (val == kth), 1.0, 0.0).astype(BF16)
                got = dot(pick, ag[:, :, :, :w].reshape(SIDE * SIDE * TOK, w)).astype(BF16).reshape(CORES, SIDE, 16, w)
                ps[there] = got
                for flip in (0, 1):
                    there_core = core if flip == 0 else 1 - core
                    if off == 0 and flip == 0:
                        pr[there, core] = ps[there, core]
                        continue
                    ops.append(links.copy(ps.at[there, there_core], pr.at[pos[d3], core], first + there_core))
        return ops

    def experts(b, ops3):
        for op in ops3:
            op.wait_recv()
        pr = b["pr"]
        xbuf[:, :WIDTHS[0]] = pr[0][...].reshape(SLOTS, WIDTHS[0])
        for cls in (1, 2):
            s, w = STARTS[cls], WIDTHS[cls]
            xbuf[:, s:s + w] = dot(perms[cls - 1], pr[cls][...].reshape(SLOTS, w)).astype(BF16)

        @pl.loop(0, FF // 256)
        def _(i):
            cols = pl.ds(pl.multiple_of(i * 256, 256), 256)
            g = dot(xbuf[...], vg[:, cols])
            u = dot(xbuf[...], vu[:, cols])
            hbuf[:, cols] = (g * (1.0 / (1.0 + jnp.exp(-g))) * u).astype(BF16)

    def back1(b):
        ops = []
        r1 = b["r1"]
        for cls, (d1, d2, d3) in enumerate(CLASSES):
            w, s = WIDTHS[cls], STARTS[cls]
            if cls == 0:
                h = hbuf[...]
            else:
                h = dot(perms[cls + 1], hbuf[...]).astype(BF16)
            y = dot(h, vd[:, s:s + w]).astype(BF16)
            ps_y = b["pr"][cls]
            ps_y[...] = y.reshape(SIDE, CORES, SIDE, 16, w)
            for off in (2, 1, 3, 0):
                there, dev = along(d3, off)
                first = dev - core
                for flip in (0, 1):
                    there_core = core if flip == 0 else 1 - core
                    if off == 0 and flip == 0:
                        r1[cls][there * CORES + core] = ps_y[there, core]
                        continue
                    ops.append(links.copy(ps_y.at[there, there_core],
                                          r1[cls].at[pos[d3] * CORES + core], first + there_core))
        return ops

    def back2(b, ops1):
        ops = []
        for cls, (d1, d2, d3) in enumerate(CLASSES):
            for op in ops1[7 * cls:7 * cls + 7]:
                op.wait_recv()
            r1, r2 = b["r1"][cls], b["r2"][cls]
            for off in (2, 1, 3):
                there, dev = along(d2, off)
                ops.append(links.copy(r1.at[:, there], r2.at[pos[d2]], dev))
            r2[pos[d2]] = r1[:, pos[d2]]
        return ops

    def back3(b, ops2):
        ops = []
        slot = iota((SLOTS, 1), 0)
        col = iota((SIDE * TOK, SLOTS), 1)
        same = ((col >> 2) & 3) == (iota((SIDE * TOK, SLOTS), 0) >> 5)
        kth = (col & 3).astype(F32)
        for cls, (d1, d2, d3) in enumerate(CLASSES):
            w = WIDTHS[cls]
            owner = (pos[d1] * STRIDE[d1] + (slot >> 7) * STRIDE[d2] + ((slot >> 5) & 3) * STRIDE[d3] + ((slot >> 4) & 1))
            pick_exp = (iota((SLOTS, N_EXP), 1) == owner).astype(F32).astype(BF16)
            ranks = b["ag"][cls][pos[d2], :, :, w:].reshape(SIDE * TOK, N_EXP)
            g = b["gg"][cls][...].reshape(SIDE * TOK, N_EXP)
            g1 = g.astype(BF16)
            rest = g - g1.astype(F32)
            g2 = rest.astype(BF16)
            g3 = (rest - g2.astype(F32)).astype(BF16)
            keep = same & (dot_nt(ranks, pick_exp) == kth)
            for op in ops2[3 * cls:3 * cls + 3]:
                op.wait_recv()
            rows = b["r2"][cls][...].reshape(SLOTS, w)
            total = None
            for part in (g3, g2, g1):
                weight = jnp.where(keep, dot_nt(part, pick_exp), 0.0).astype(BF16)
                term = dot(weight, rows)
                total = term if total is None else total + term
            sm, r3 = b["sm"][cls], b["r3"][cls]
            sm[...] = total.reshape(SIDE, TOK, w)
            for off in (2, 1, 3):
                there, dev = along(d1, off)
                ops.append(links.copy(sm.at[there], r3.at[pos[d1]], dev))
            r3[pos[d1]] = sm[pos[d1]]
        return ops

    def finish(b, ops3, rows, out):
        for cls in range(3):
            w, s = WIDTHS[cls], STARTS[cls]
            for op in ops3[3 * cls:3 * cls + 3]:
                op.wait_recv()
            r3 = b["r3"][cls]
            total = (r3[0] + r3[1]) + (r3[2] + r3[3])
            out[:, s:s + w] = (rows[:, s:s + w].astype(F32) + total).astype(BF16)

    a, b = bufs
    prepare(a, x_a, route_a, gate_a)
    pl.semaphore_wait(barrier, len(peers))
    a1 = gather1(a)
    for i in range(4):
        proj_step(i)
    a2 = gather2(a, a1)
    for i in range(4, n_wo):
        proj_step(i)
    u_b[...] = (h_b[...].astype(F32) + proj_acc[...].astype(BF16).astype(F32)).astype(BF16)
    prepare(b, u_b, route_b, gate_b)
    b1 = gather1(b)
    perms[0] = reorder(0, 1)
    perms[1] = reorder(0, 2)
    perms[2] = reorder(1, 0)
    perms[3] = reorder(2, 0)
    b2 = gather2(b, b1)
    ag_gates = gather_gates(a)
    bg_gates = gather_gates(b)
    a3 = exchange(a, a2)
    for i in range(4):
        qkv_step(i)
    b3 = exchange(b, b2)
    for i in range(4, n_wq):
        qkv_step(i)
    for c in w_copies:
        c.wait()
    experts(a, a3)
    a4 = back1(a)
    experts(b, b3)
    b4 = back1(b)
    for op in ag_gates + bg_gates:
        op.wait_recv()
    a5 = back2(a, a4)
    b5 = back2(b, b4)
    a6 = back3(a, a5)
    b6 = back3(b, b5)
    finish(a, a6, x_a, out_a)
    finish(b, b6, u_b, out_b)
    links.drain()


def solution(mesh):
    def local_step(x_a, route_a, gate_a, h_b, attn_b, route_b, gate_b, w_qkv, w_o, w_gate, w_up, w_down):
        vmem = pl.BlockSpec(memory_space=pltpu.VMEM)
        hbm = pl.BlockSpec(memory_space=pl.ANY)
        scratch = []
        for _ in range(2):
            for shape, dtype in (
                (lambda w: (SIDE, SIDE, TOK, w + N_EXP), BF16),
                (lambda w: (SIDE, CORES, SIDE, 16, w), BF16),
                (lambda w: (SIDE, CORES, SIDE, 16, w), BF16),
                (lambda w: (SIDE * CORES, SIDE, 16, w), BF16),
                (lambda w: (SIDE, SIDE * CORES, 16, w), BF16),
                (lambda w: (SIDE, TOK, w), F32),
                (lambda w: (SIDE, TOK, w), F32),
                (lambda w: (SIDE, TOK, N_EXP), F32),
            ):
                scratch += [pltpu.VMEM(shape(w), dtype) for w in WIDTHS]
        scratch += [
            pltpu.VMEM((SLOTS, D), BF16),
            pltpu.VMEM((SLOTS, FF), BF16),
            pltpu.VMEM((4, SLOTS, SLOTS), BF16),
            pltpu.VMEM((TOK, D), F32),
            pltpu.VMEM((TOK, QKV), F32),
            pltpu.VMEM((TOK, D), BF16),
            pltpu.VMEM((D, FF), BF16),
            pltpu.VMEM((D, FF), BF16),
            pltpu.VMEM((FF, D), BF16),
            pltpu.VMEM((2, WO_CHUNK, D), BF16),
            pltpu.VMEM((2, WQ_CHUNK, QKV), BF16),
            pltpu.SemaphoreType.DMA((n_copies(),)),
            pltpu.SemaphoreType.DMA((n_copies(),)),
            pltpu.SemaphoreType.DMA((3,)),
            pltpu.SemaphoreType.DMA((2,)),
            pltpu.SemaphoreType.DMA((2,)),
        ]
        return pl.pallas_call(
            kernel,
            out_shape=(
                jax.ShapeDtypeStruct((TOK, D), BF16),
                jax.ShapeDtypeStruct((TOK, D), BF16),
                jax.ShapeDtypeStruct((TOK, QKV), BF16),
            ),
            in_specs=[vmem] * 7 + [hbm] * 5,
            out_specs=(vmem, vmem, vmem),
            scratch_shapes=scratch,
            name="moe_pair",
            compiler_params=pltpu.CompilerParams(
                collective_id=0, has_side_effects=True, vmem_limit_bytes=64 * 2**20 - 2**16),
        )(x_a, h_b, attn_b, route_a, route_b, gate_a, gate_b, w_qkv, w_o, w_gate, w_up, w_down)

    row_spec = P(("dp", "ep"), None)
    full_spec = P(None, None)
    expert_spec = P("ep", None, None)
    return jax.shard_map(
        local_step,
        mesh=mesh,
        in_specs=(row_spec,) * 7 + (full_spec, full_spec) + (expert_spec,) * 3,
        out_specs=(row_spec, row_spec, row_spec),
        check_vma=False,
    )
```

```python
import jax
import jax.numpy as jnp
from jax import lax
from jax.experimental import pallas as pl
from jax.experimental.pallas import tpu as pltpu
from jax.sharding import PartitionSpec as P

MESH = pl.DeviceIdType.MESH
BF16 = jnp.bfloat16
F32 = jnp.float32

SIDE = 4
CORES = 2
TOK = 32
CAP = 4
TOP_K = 8
D = 2048
N_EXP = 128
FF = 768
ATT = 4096
QKV = 5120
SLOTS = N_EXP * CAP
CLASSES = ((0, 1, 2), (1, 2, 0), (2, 0, 1))
WIDTHS = ((768, 640, 640), (640, 768, 640))
STARTS = ((0, 768, 1408), (0, 640, 1408))
STRIDE = (32, 8, 2)
UNUSED = 8.0
WO_CHUNK = 512
WQ_CHUNK = 256
HALF = SLOTS // 2
COLUMN = SIDE * TOK


def iota(shape, dim):
    return lax.broadcasted_iota(jnp.int32, shape, dim)


def ones_where(cond):
    return jnp.where(cond, 1.0, 0.0).astype(BF16)


def dot(a, b):
    return jnp.dot(a, b, preferred_element_type=F32)


def dot_nt(a, b):
    return lax.dot_general(a, b, (((1,), (1,)), ((), ())), preferred_element_type=F32)


def reorder(to_cls, from_cls):
    row = iota((HALF, 1), 0)
    d1, d2, d3 = CLASSES[to_cls]
    coords = {d3: row >> 6, d2: (row >> 4) & 3, d1: (row >> 2) & 3}
    d1, d2, d3 = CLASSES[from_cls]
    want = (coords[d3] << 6) | (coords[d2] << 4) | (coords[d1] << 2) | (row & 3)
    return ones_where(iota((HALF, HALF), 1) == want)


class Links:
    def __init__(self, send, recv):
        self.send, self.recv, self.open = send, recv, []

    def copy(self, src, dst, device):
        i = len(self.open)
        op = pltpu.make_async_remote_copy(
            src_ref=src, dst_ref=dst, send_sem=self.send.at[i], recv_sem=self.recv.at[i],
            device_id={"ep": device}, device_id_type=MESH)
        op.start()
        self.open.append(op)
        return op

    def drain(self):
        for op in self.open:
            op.wait_send()


def arrived(ops):
    for op in ops:
        op.wait_recv()


N_COPIES = 18 + 2 * (9 + 12 + 84 + 21 + 36 + 9)


def kernel(*refs):
    it = iter(refs)
    take = lambda n: [next(it) for _ in range(n)]
    x_a, h_b, attn, route_a, route_b, gate_a, gate_b = take(7)
    w_qkv, w_o, w_gate, w_up, w_down = take(5)
    out_a, out_b, qkv_out = take(3)
    batches = []
    for m in range(2):
        b = {"m": m, "w": WIDTHS[m], "s": STARTS[m]}
        for name in ("ag", "ps", "pr", "r1", "r2", "sm", "r3"):
            b[name] = take(3)
        batches.append(b)
    meta, routes, gates = take(3), take(3), take(3)
    xbuf, hbuf, perms, proj_acc, qkv_acc, u_b = take(6)
    vg, vu, vd, wo_buf, wq_buf = take(5)
    send_sem, recv_sem, w_sem, wo_sem, wq_sem = take(5)

    me = lax.axis_index("ep")
    core = lax.rem(me, 2)
    pos = [lax.rem(me // 32, 4), lax.rem(me // 8, 4), lax.rem(me // 2, 4)]
    links = Links(send_sem, recv_sem)

    def along(dim, off):
        there = lax.rem(pos[dim] + off, 4)
        return there, me + (there - pos[dim]) * STRIDE[dim]

    peers = []
    for dim in range(3):
        for off in (1, 2, 3):
            _, dev = along(dim, off)
            peers += [dev, dev + 1 - 2 * core]
    peers.append(me + 1 - 2 * core)
    barrier = pltpu.get_barrier_semaphore()
    for dev in peers:
        pl.semaphore_signal(barrier, inc=1, device_id={"ep": dev}, device_id_type=MESH)

    w_copies = [pltpu.make_async_copy(src.at[0], dst, w_sem.at[i])
                for i, (src, dst) in enumerate(((w_gate, vg), (w_up, vu), (w_down, vd)))]
    n_wo, n_wq = ATT // WO_CHUNK, D // WQ_CHUNK

    def wo_copy(i):
        return pltpu.make_async_copy(w_o.at[pl.ds(i * WO_CHUNK, WO_CHUNK)], wo_buf.at[i % 2], wo_sem.at[i % 2])

    def wq_copy(i):
        return pltpu.make_async_copy(w_qkv.at[pl.ds(i * WQ_CHUNK, WQ_CHUNK)], wq_buf.at[i % 2], wq_sem.at[i % 2])

    wo_copy(0).start()
    wo_copy(1).start()
    for c in w_copies:
        c.start()
    wq_copy(0).start()
    wq_copy(1).start()

    def proj_step(i):
        wo_copy(i).wait()
        part = dot(attn[:, i * WO_CHUNK:(i + 1) * WO_CHUNK], wo_buf[i % 2])
        proj_acc[...] = part if i == 0 else proj_acc[...] + part
        if i + 2 < n_wo:
            wo_copy(i + 2).start()

    def qkv_step(i):
        wq_copy(i).wait()
        part = dot(h_b[:, i * WQ_CHUNK:(i + 1) * WQ_CHUNK], wq_buf[i % 2])
        if i == n_wq - 1:
            qkv_out[...] = (qkv_acc[...] + part).astype(BF16)
        else:
            qkv_acc[...] = part if i == 0 else qkv_acc[...] + part
        if i + 2 < n_wq:
            wq_copy(i + 2).start()

    earlier = ones_where((iota((COLUMN, COLUMN), 0) < iota((COLUMN, COLUMN), 1))
                         & (iota((COLUMN, COLUMN), 0) >> 5 == iota((COLUMN, COLUMN), 1) >> 5))

    def rank_of(route, expert):
        hit = route[0:1] == expert
        for j in range(1, TOP_K):
            hit = hit | (route[j:j + 1] == expert)
        rank = dot(ones_where(hit), earlier)
        return jnp.where(hit, rank, UNUSED)

    def write_meta():
        for cls, (d1, d2, d3) in enumerate(CLASSES):
            for i, (a, b) in enumerate(((route_a, route_b), (gate_a, gate_b))):
                meta[cls][pos[d1], i] = jnp.zeros((TOP_K, N_EXP), F32)
                meta[cls][pos[d1], i, :, 0:TOK] = a[...].astype(F32)
                meta[cls][pos[d1], i, :, TOK:2 * TOK] = b[...].astype(F32)

    def send_meta1():
        ops = []
        for cls, (d1, d2, d3) in enumerate(CLASSES):
            mine = meta[cls].at[pos[d1]]
            for off in (2, 1, 3):
                ops.append(links.copy(mine, mine, along(d1, off)[1]))
        return ops

    def send_meta2(ops1):
        lane = iota((TOP_K, COLUMN), 1) >> 5
        ops = []
        for cls, (d1, d2, d3) in enumerate(CLASSES):
            arrived(ops1[3 * cls:3 * cls + 3])
            for i, dst in ((0, routes[cls].at[pos[d2]]), (1, gates[cls])):
                for m in range(2):
                    packed = jnp.zeros((TOP_K, COLUMN), F32)
                    for v in range(SIDE):
                        shift = (TOK * (v - m)) % COLUMN
                        piece = meta[cls][v, i]
                        packed = jnp.where(lane == v, pltpu.roll(piece, shift, 1) if shift else piece, packed)
                    dst[m] = packed
            mine = routes[cls].at[pos[d2]]
            for off in (2, 1, 3):
                ops.append(links.copy(mine, mine, along(d2, off)[1]))
        return ops

    def gather1(b, rows):
        ops = []
        for cls, (d1, d2, d3) in enumerate(CLASSES):
            w, s = b["w"][cls], b["s"][cls]
            for off in (2, 1, 3):
                ops.append(links.copy(rows.at[:, s:s + w], b["ag"][cls].at[pos[d2], pos[d1]], along(d1, off)[1]))
        for cls, (d1, d2, d3) in enumerate(CLASSES):
            w, s = b["w"][cls], b["s"][cls]
            b["ag"][cls][pos[d2], pos[d1]] = rows[:, s:s + w]
        return ops

    def gather2(b, ops1):
        ops = []
        for cls, (d1, d2, d3) in enumerate(CLASSES):
            arrived(ops1[3 * cls:3 * cls + 3])
            mine = b["ag"][cls].at[pos[d2]]
            for off in (1, 3):
                ops.append(links.copy(mine, mine, along(d2, off)[1]))
        return ops

    def relay2(b, ops2):
        ops = []
        for cls, (d1, d2, d3) in enumerate(CLASSES):
            arrived(ops2[2 * cls:2 * cls + 2])
            for off, half in ((1, 0), (3, 2)):
                got = b["ag"][cls].at[along(d2, 4 - off)[0], half:half + 2]
                ops.append(links.copy(got, got, along(d2, off)[1]))
        return ops

    def pick(b, cls, off2):
        d1, d2, d3 = CLASSES[cls]
        w = b["w"][cls]
        block = along(d2, off2)[0]
        exp = iota((SIDE * CORES, 1), 0)
        exp = me - pos[d3] * STRIDE[d3] - core + (exp >> 1) * STRIDE[d3] + (exp & 1)
        rank = rank_of(routes[cls][block, b["m"]], exp.astype(F32))
        rank = jnp.concatenate([jnp.broadcast_to(rank[e:e + 1], (16, COLUMN)) for e in range(SIDE * CORES)], axis=0)
        slot = iota((COLUMN, 1), 0)
        mask = ((slot >> 2) & 3) == (iota((COLUMN, COLUMN), 1) >> 5)
        choice = ones_where(mask & (rank == (slot & 3).astype(F32)))
        got = dot(choice, b["ag"][cls][block].reshape(COLUMN, w)).astype(BF16)
        ps, pr = b["ps"][cls], b["pr"][cls]
        ps[block] = got.reshape(SIDE, CORES, 16, w)
        ops = []
        for off in (2, 1, 3, 0):
            there, dev = along(d3, off)
            first = dev - core
            for flip in (0, 1):
                there_core = core if flip == 0 else 1 - core
                if off == 0 and flip == 0:
                    pr[there, core, block] = ps[block, there, core]
                    continue
                ops.append(links.copy(ps.at[block, there, there_core], pr.at[pos[d3], core, block], first + there_core))
        return ops

    def experts(b, ops3):
        arrived(ops3)
        pr = b["pr"]
        for cls in range(3):
            s, w = b["s"][cls], b["w"][cls]
            for c in range(CORES):
                rows = pr[cls][:, c].reshape(HALF, w)
                if cls:
                    rows = dot(perms[cls - 1], rows).astype(BF16)
                xbuf[:, c, :, s:s + w] = rows.reshape(SIDE, 64, w)

        @pl.loop(0, FF // 256)
        def _(i):
            cols = pl.ds(pl.multiple_of(i * 256, 256), 256)
            x = xbuf[...].reshape(SLOTS, D)
            g = dot(x, vg[:, cols])
            u = dot(x, vu[:, cols])
            h = (g * (1.0 / (1.0 + jnp.exp(-g))) * u).astype(BF16)
            hbuf[:, :, :, cols] = h.reshape(SIDE, CORES, 64, 256)

    def back1(b):
        ops = []
        for cls, (d1, d2, d3) in enumerate(CLASSES):
            w, s = b["w"][cls], b["s"][cls]
            r1, y = b["r1"][cls], b["pr"][cls]
            for c in range(CORES):
                h = hbuf[:, c].reshape(HALF, FF)
                if cls:
                    h = dot(perms[cls + 1], h).astype(BF16)
                y[:, c] = dot(h, vd[:, s:s + w]).astype(BF16).reshape(SIDE, SIDE, 16, w)
            for off in (2, 1, 3, 0):
                there, dev = along(d3, off)
                first = dev - core
                for flip in (0, 1):
                    there_core = core if flip == 0 else 1 - core
                    if off == 0 and flip == 0:
                        r1[there, core] = y[there, core]
                        continue
                    ops.append(links.copy(y.at[there, there_core], r1.at[pos[d3], core], first + there_core))
        return ops

    def back2(b, ops1):
        ops = []
        for cls, (d1, d2, d3) in enumerate(CLASSES):
            r1, r2 = b["r1"][cls], b["r2"][cls]
            mine = ops1[7 * cls:7 * cls + 7]
            for off, got in ((0, mine[6:7]), (3, mine[2:4]), (1, mine[4:6]), (2, mine[0:2])):
                arrived(got)
                chip = along(d3, off)[0]
                for to in (2, 1, 3):
                    there, dev = along(d2, to)
                    ops.append(links.copy(r1.at[chip, :, there], r2.at[pos[d2], chip], dev))
                r2[pos[d2], chip] = r1[chip, :, pos[d2]]
        return ops

    def weights(b, cls):
        d1, d2, d3 = CLASSES[cls]
        m = b["m"]
        route = routes[cls][pos[d2], m]
        gate = gates[cls][m]
        exp = iota((N_EXP, 1), 0).astype(F32)
        rank = rank_of(route, exp)
        value = jnp.zeros((N_EXP, COLUMN), F32)
        for j in range(TOP_K):
            value = jnp.where(route[j:j + 1] == exp, gate[j:j + 1], value)
        rank, value = rank.T.astype(BF16), value.T
        slot = iota((SLOTS, 1), 0)
        owner = pos[d1] * STRIDE[d1] + (slot >> 7) * STRIDE[d2] + ((slot >> 5) & 3) * STRIDE[d3] + ((slot >> 4) & 1)
        onehot = ones_where(iota((SLOTS, N_EXP), 1) == owner)
        col = iota((COLUMN, SLOTS), 1)
        keep = ((col >> 2) & 3) == (iota((COLUMN, SLOTS), 0) >> 5)
        keep = keep & (dot_nt(rank, onehot) == (col & 3).astype(F32))
        part1 = value.astype(BF16)
        rest = value - part1.astype(F32)
        part2 = rest.astype(BF16)
        part3 = (rest - part2.astype(F32)).astype(BF16)
        return jnp.concatenate(
            [jnp.where(keep, dot_nt(part, onehot), 0.0).astype(BF16) for part in (part3, part2, part1)], axis=0)

    def back3(b, ops2):
        ops = []
        for cls, (d1, d2, d3) in enumerate(CLASSES):
            w = b["w"][cls]
            weight = weights(b, cls)
            arrived(ops2[12 * cls:12 * cls + 12])
            terms = dot(weight, b["r2"][cls][...].reshape(SLOTS, w)).reshape(3, COLUMN, w)
            sm, r3 = b["sm"][cls], b["r3"][cls]
            sm[...] = ((terms[0] + terms[1]) + terms[2]).reshape(SIDE, TOK, w)
            for off in (2, 1, 3):
                there, dev = along(d1, off)
                ops.append(links.copy(sm.at[there], r3.at[pos[d1]], dev))
            r3[pos[d1]] = sm[pos[d1]]
        return ops

    def finish(b, ops3, rows, out):
        for cls in range(3):
            w, s = b["w"][cls], b["s"][cls]
            arrived(ops3[3 * cls:3 * cls + 3])
            r3 = b["r3"][cls]
            total = (r3[0] + r3[1]) + (r3[2] + r3[3])
            out[:, s:s + w] = (rows[:, s:s + w].astype(F32) + total).astype(BF16)

    a, b = batches
    write_meta()
    pl.semaphore_wait(barrier, len(peers))
    a1 = gather1(a, x_a)
    m1 = send_meta1()
    proj_step(0)
    proj_step(1)
    a2 = gather2(a, a1)
    m2 = send_meta2(m1)
    proj_step(2)
    a3 = []
    for cls in range(3):
        a3 += pick(a, cls, 0)
    proj_step(3)
    proj_step(4)
    ar = relay2(a, a2)
    proj_step(5)
    arrived(m2)
    for cls in range(3):
        a3 += pick(a, cls, 1)
    proj_step(6)
    for cls in range(3):
        a3 += pick(a, cls, 3)
    proj_step(7)
    u_b[...] = (h_b[...].astype(F32) + proj_acc[...].astype(BF16).astype(F32)).astype(BF16)
    b1 = gather1(b, u_b)
    for cls in range(3):
        arrived(ar[2 * cls:2 * cls + 2])
        a3 += pick(a, cls, 2)
    b2 = gather2(b, b1)
    perms[0] = reorder(0, 1)
    perms[1] = reorder(0, 2)
    perms[2] = reorder(1, 0)
    perms[3] = reorder(2, 0)
    b3 = []
    for cls in range(3):
        b3 += pick(b, cls, 0)
    qkv_step(0)
    br = relay2(b, b2)
    for cls in range(3):
        b3 += pick(b, cls, 1)
        b3 += pick(b, cls, 3)
    qkv_step(1)
    for cls in range(3):
        arrived(br[2 * cls:2 * cls + 2])
        b3 += pick(b, cls, 2)
    for c in w_copies:
        c.wait()
    experts(a, a3)
    a4 = back1(a)
    experts(b, b3)
    b4 = back1(b)
    a5 = back2(a, a4)
    for i in range(2, 5):
        qkv_step(i)
    b5 = back2(b, b4)
    for i in range(5, n_wq):
        qkv_step(i)
    a6 = back3(a, a5)
    b6 = back3(b, b5)
    finish(a, a6, x_a, out_a)
    finish(b, b6, u_b, out_b)
    links.drain()


def deliver(*refs):
    n = (len(refs) - 1) // 2
    ops = [pltpu.make_async_copy(refs[i], refs[n + i], refs[-1].at[i]) for i in range(n)]
    for op in ops:
        op.start()
    for op in ops:
        op.wait()


def solution(mesh):
    def local_step(x_a, route_a, gate_a, h_b, attn_b, route_b, gate_b, w_qkv, w_o, w_gate, w_up, w_down):
        vmem = pl.BlockSpec(memory_space=pltpu.VMEM)
        hbm = pl.BlockSpec(memory_space=pl.ANY)
        scratch = []
        for m in range(2):
            for shape, dtype in (
                (lambda w: (SIDE, SIDE, TOK, w), BF16),
                (lambda w: (SIDE, SIDE, CORES, 16, w), BF16),
                (lambda w: (SIDE, CORES, SIDE, 16, w), BF16),
                (lambda w: (SIDE, CORES, SIDE, 16, w), BF16),
                (lambda w: (SIDE, SIDE, CORES, 16, w), BF16),
                (lambda w: (SIDE, TOK, w), F32),
                (lambda w: (SIDE, TOK, w), F32),
            ):
                scratch += [pltpu.VMEM(shape(w), dtype) for w in WIDTHS[m]]
        scratch += [pltpu.VMEM((SIDE, 2, TOP_K, COLUMN), F32)] * 3
        scratch += [pltpu.VMEM((SIDE, 2, TOP_K, COLUMN), F32)] * 3
        scratch += [pltpu.VMEM((2, TOP_K, COLUMN), F32)] * 3
        scratch += [
            pltpu.VMEM((SIDE, CORES, 64, D), BF16),
            pltpu.VMEM((SIDE, CORES, 64, FF), BF16),
            pltpu.VMEM((4, HALF, HALF), BF16),
            pltpu.VMEM((TOK, D), F32),
            pltpu.VMEM((TOK, QKV), F32),
            pltpu.VMEM((TOK, D), BF16),
            pltpu.VMEM((D, FF), BF16),
            pltpu.VMEM((D, FF), BF16),
            pltpu.VMEM((FF, D), BF16),
            pltpu.VMEM((2, WO_CHUNK, D), BF16),
            pltpu.VMEM((2, WQ_CHUNK, QKV), BF16),
            pltpu.SemaphoreType.DMA((N_COPIES,)),
            pltpu.SemaphoreType.DMA((N_COPIES,)),
            pltpu.SemaphoreType.DMA((3,)),
            pltpu.SemaphoreType.DMA((2,)),
            pltpu.SemaphoreType.DMA((2,)),
        ]
        outs = tuple(jax.ShapeDtypeStruct((TOK, n), BF16) for n in (D, D, QKV))
        results = pl.pallas_call(
            kernel,
            out_shape=outs,
            in_specs=[vmem] * 7 + [hbm] * 5,
            out_specs=(vmem,) * 3,
            scratch_shapes=scratch,
            name="moe_pair",
            compiler_params=pltpu.CompilerParams(
                collective_id=0, has_side_effects=True, vmem_limit_bytes=64 * 2**20 - 2**16),
        )(x_a, h_b, attn_b, route_a.T, route_b.T, gate_a.T, gate_b.T, w_qkv, w_o, w_gate, w_up, w_down)
        return pl.pallas_call(
            deliver,
            out_shape=outs,
            in_specs=[hbm] * 3,
            out_specs=(vmem,) * 3,
            scratch_shapes=[pltpu.SemaphoreType.DMA((3,))],
            name="deliver",
        )(*results)

    row_spec = P(("dp", "ep"), None)
    full_spec = P(None, None)
    expert_spec = P("ep", None, None)
    return jax.shard_map(
        local_step,
        mesh=mesh,
        in_specs=(row_spec,) * 7 + (full_spec, full_spec) + (expert_spec,) * 3,
        out_specs=(row_spec, row_spec, row_spec),
        check_vma=False,
    )
```

```python
import jax
import jax.numpy as jnp
from jax import lax
from jax.experimental import pallas as pl
from jax.experimental.pallas import tpu as pltpu
from jax.sharding import PartitionSpec as P

MESH = pl.DeviceIdType.MESH
BF16 = jnp.bfloat16
F32 = jnp.float32

SIDE = 4
CORES = 2
TOK = 32
CAP = 4
TOP_K = 8
D = 2048
N_EXP = 128
FF = 768
ATT = 4096
QKV = 5120
SLOTS = N_EXP * CAP
CLASSES = ((0, 1, 2), (1, 2, 0), (2, 0, 1))
WIDTHS = ((768, 640, 640), (640, 768, 640))
STARTS = ((0, 768, 1408), (0, 640, 1408))
STRIDE = (32, 8, 2)
UNUSED = 8.0
WO_CHUNK = 512
WQ_CHUNK = 256
HALF = SLOTS // 2
COLUMN = SIDE * TOK


def iota(shape, dim):
    return lax.broadcasted_iota(jnp.int32, shape, dim)


def ones_where(cond):
    return jnp.where(cond, 1.0, 0.0).astype(BF16)


def dot(a, b):
    return jnp.dot(a, b, preferred_element_type=F32)


def dot_nt(a, b):
    return lax.dot_general(a, b, (((1,), (1,)), ((), ())), preferred_element_type=F32)


def reorder(to_cls, from_cls):
    row = iota((HALF, 1), 0)
    d1, d2, d3 = CLASSES[to_cls]
    coords = {d3: row >> 6, d2: (row >> 4) & 3, d1: (row >> 2) & 3}
    d1, d2, d3 = CLASSES[from_cls]
    want = (coords[d3] << 6) | (coords[d2] << 4) | (coords[d1] << 2) | (row & 3)
    return ones_where(iota((HALF, HALF), 1) == want)


class Links:
    def __init__(self, send, recv, other):
        self.send, self.recv, self.other, self.sends, self.recvs = send, recv, other, {}, {}

    def _op(self, src, dst, device, phase, group):
        i = self.sends.setdefault(phase, len(self.sends))
        j = self.recvs.setdefault(group, len(self.recvs))
        return pltpu.make_async_remote_copy(
            src_ref=src, dst_ref=dst, send_sem=self.send.at[i], recv_sem=self.recv.at[j],
            device_id={"ep": device}, device_id_type=MESH)

    def copy(self, src, dst, device, phase, *rest):
        self._op(src, dst, device, phase, phase + rest).start()

    def arrived(self, like, phase, *rest):
        self._op(like, like, self.other, phase, phase + rest).wait_recv()

    def sent(self, like, phase):
        self._op(like, like, self.other, phase, next(g for g in self.recvs if g[:len(phase)] == phase)).wait_send()


N_PHASES = 6 + 2 * 21
N_GROUPS = 6 + 2 * (3 + 3 + 3 + 3 + 24 + 6 + 6)
FIRST = 384


def kernel(*refs):
    it = iter(refs)
    take = lambda n: [next(it) for _ in range(n)]
    x_a, h_b, attn, route_a, route_b, gate_a, gate_b = take(7)
    w_qkv, w_o, w_gate, w_up, w_down = take(5)
    out_a, out_b, qkv_out = take(3)
    batches = []
    for m in range(2):
        b = {"m": m, "w": WIDTHS[m], "s": STARTS[m]}
        for name in ("ag", "ps", "pr", "r1", "r2", "sm", "r3"):
            b[name] = take(3)
        batches.append(b)
    meta, routes, gates = take(3), take(3), take(3)
    xbuf, hbuf, hperm, wts, perms, proj_acc, qkv_acc, u_b = take(8)
    vg, vu, vd, wo_buf, wq_buf = take(5)
    send_sem, recv_sem, w_sem, wo_sem, wq_sem = take(5)

    me = lax.axis_index("ep")
    core = lax.rem(me, 2)
    pos = [lax.rem(me // 32, 4), lax.rem(me // 8, 4), lax.rem(me // 2, 4)]
    links = Links(send_sem, recv_sem, me + 1 - 2 * core)

    def along(dim, off):
        there = lax.rem(pos[dim] + off, 4)
        return there, me + (there - pos[dim]) * STRIDE[dim]

    peers = []
    for dim in range(3):
        for off in (1, 2, 3):
            _, dev = along(dim, off)
            peers += [dev, dev + 1 - 2 * core]
    peers.append(me + 1 - 2 * core)
    barrier = pltpu.get_barrier_semaphore()
    for dev in peers:
        pl.semaphore_signal(barrier, inc=1, device_id={"ep": dev}, device_id_type=MESH)

    w_copies = [pltpu.make_async_copy(src.at[0], dst, w_sem.at[i])
                for i, (src, dst) in enumerate(((w_gate, vg), (w_up, vu), (w_down, vd)))]
    n_wo, n_wq = ATT // WO_CHUNK, D // WQ_CHUNK

    def wo_copy(i):
        return pltpu.make_async_copy(w_o.at[pl.ds(i * WO_CHUNK, WO_CHUNK)], wo_buf.at[i % 2], wo_sem.at[i % 2])

    def wq_copy(i):
        return pltpu.make_async_copy(w_qkv.at[pl.ds(i * WQ_CHUNK, WQ_CHUNK)], wq_buf.at[i % 2], wq_sem.at[i % 2])

    wo_copy(0).start()
    wo_copy(1).start()
    for c in w_copies:
        c.start()
    wq_copy(0).start()
    wq_copy(1).start()

    def proj_step(i):
        wo_copy(i).wait()
        part = dot(attn[:, i * WO_CHUNK:(i + 1) * WO_CHUNK], wo_buf[i % 2])
        proj_acc[...] = part if i == 0 else proj_acc[...] + part
        if i + 2 < n_wo:
            wo_copy(i + 2).start()

    def qkv_step(i):
        wq_copy(i).wait()
        part = dot(h_b[:, i * WQ_CHUNK:(i + 1) * WQ_CHUNK], wq_buf[i % 2])
        if i == n_wq - 1:
            qkv_out[...] = (qkv_acc[...] + part).astype(BF16)
        else:
            qkv_acc[...] = part if i == 0 else qkv_acc[...] + part
        if i + 2 < n_wq:
            wq_copy(i + 2).start()

    earlier = ones_where((iota((COLUMN, COLUMN), 0) < iota((COLUMN, COLUMN), 1))
                         & (iota((COLUMN, COLUMN), 0) >> 5 == iota((COLUMN, COLUMN), 1) >> 5))

    def rank_of(route, expert):
        hit = route[0:1] == expert
        for j in range(1, TOP_K):
            hit = hit | (route[j:j + 1] == expert)
        rank = dot(ones_where(hit), earlier)
        return jnp.where(hit, rank, UNUSED)

    def write_meta():
        for cls, (d1, d2, d3) in enumerate(CLASSES):
            for i, (a, b) in enumerate(((route_a, route_b), (gate_a, gate_b))):
                meta[cls][pos[d1], i] = jnp.zeros((TOP_K, N_EXP), F32)
                meta[cls][pos[d1], i, :, 0:TOK] = a[...].astype(F32)
                meta[cls][pos[d1], i, :, TOK:2 * TOK] = b[...].astype(F32)

    def send_meta1():
        for cls, (d1, d2, d3) in enumerate(CLASSES):
            mine = meta[cls].at[pos[d1]]
            for off in (2, 1, 3):
                links.copy(mine, mine, along(d1, off)[1], ("meta1", cls))

    def send_meta2():
        lane = iota((TOP_K, COLUMN), 1) >> 5
        for cls, (d1, d2, d3) in enumerate(CLASSES):
            links.arrived(meta[cls].at[0:3], ("meta1", cls))
            for i, dst in ((0, routes[cls].at[pos[d2]]), (1, gates[cls])):
                for m in range(2):
                    packed = jnp.zeros((TOP_K, COLUMN), F32)
                    for v in range(SIDE):
                        shift = (TOK * (v - m)) % COLUMN
                        piece = meta[cls][v, i]
                        packed = jnp.where(lane == v, pltpu.roll(piece, shift, 1) if shift else piece, packed)
                    dst[m] = packed
            mine = routes[cls].at[pos[d2]]
            for off in (2, 1, 3):
                links.copy(mine, mine, along(d2, off)[1], ("meta2", cls))

    def gather1(b, rows):
        for cls, (d1, d2, d3) in enumerate(CLASSES):
            w, s = b["w"][cls], b["s"][cls]
            for off in (2, 1, 3):
                links.copy(rows.at[:, s:s + w], b["ag"][cls].at[pos[d2], pos[d1]], along(d1, off)[1],
                           ("gather1", b["m"], cls))
        for cls, (d1, d2, d3) in enumerate(CLASSES):
            w, s = b["w"][cls], b["s"][cls]
            b["ag"][cls][pos[d2], pos[d1]] = rows[:, s:s + w]

    def gather2(b):
        for cls, (d1, d2, d3) in enumerate(CLASSES):
            ag = b["ag"][cls]
            links.arrived(ag.at[0, 0:3], ("gather1", b["m"], cls))
            mine = ag.at[pos[d2]]
            for off in (1, 3):
                links.copy(mine, mine, along(d2, off)[1], ("gather2", b["m"], cls))

    def relay2(b):
        for cls, (d1, d2, d3) in enumerate(CLASSES):
            ag = b["ag"][cls]
            links.arrived(ag.at[0:2], ("gather2", b["m"], cls))
            for off, half in ((1, 0), (3, 2)):
                got = ag.at[along(d2, 4 - off)[0], half:half + 2]
                links.copy(got, got, along(d2, off)[1], ("relay2", b["m"], cls))

    def relayed(b, cls):
        links.arrived(b["ag"][cls].at[0], ("relay2", b["m"], cls))

    def pick(b, cls, off2):
        d1, d2, d3 = CLASSES[cls]
        w = b["w"][cls]
        block = along(d2, off2)[0]
        exp = iota((SIDE * CORES, 1), 0)
        exp = me - pos[d3] * STRIDE[d3] - core + (exp >> 1) * STRIDE[d3] + (exp & 1)
        rank = rank_of(routes[cls][block, b["m"]], exp.astype(F32))
        rank = jnp.concatenate([jnp.broadcast_to(rank[e:e + 1], (16, COLUMN)) for e in range(SIDE * CORES)], axis=0)
        slot = iota((COLUMN, 1), 0)
        mask = ((slot >> 2) & 3) == (iota((COLUMN, COLUMN), 1) >> 5)
        choice = ones_where(mask & (rank == (slot & 3).astype(F32)))
        got = dot(choice, b["ag"][cls][block].reshape(COLUMN, w)).astype(BF16)
        ps, pr = b["ps"][cls], b["pr"][cls]
        ps[block] = got.reshape(SIDE, CORES, 16, w)
        for off in (2, 1, 3, 0):
            there, dev = along(d3, off)
            first = dev - core
            for flip in (0, 1):
                there_core = core if flip == 0 else 1 - core
                if off == 0 and flip == 0:
                    pr[CORES * there + core, block] = ps[block, there, core]
                    continue
                links.copy(ps.at[block, there, there_core], pr.at[CORES * pos[d3] + core, block], first + there_core,
                           ("pick", b["m"], cls))

    def experts(b):
        for cls in range(3):
            s, w = b["s"][cls], b["w"][cls]
            pr = b["pr"][cls]
            links.arrived(pr.at[0:7], ("pick", b["m"], cls))
            for c in range(CORES):
                rows = jnp.concatenate([pr[CORES * v + c].reshape(64, w) for v in range(SIDE)], axis=0)
                if cls:
                    rows = dot(perms[cls - 1], rows).astype(BF16)
                xbuf[:, c, :, s:s + w] = rows.reshape(SIDE, 64, w)

        @pl.loop(0, FF // 256)
        def _(i):
            cols = pl.ds(pl.multiple_of(i * 256, 256), 256)
            x = xbuf[...].reshape(SLOTS, D)
            g = dot(x, vg[:, cols])
            u = dot(x, vu[:, cols])
            h = (g * (1.0 / (1.0 + jnp.exp(-g))) * u).astype(BF16)
            hbuf[:, :, :, cols] = h.reshape(SIDE, CORES, 64, 256)

    def lanes(b, cls, part):
        return (0, FIRST) if part == 0 else (FIRST, b["w"][cls])

    def align(b):
        for cls in (1, 2):
            for c in range(CORES):
                hperm[cls - 1, c] = dot(perms[cls + 1], hbuf[:, c].reshape(HALF, FF)).astype(BF16)

    def back1(b, part):
        for cls, (d1, d2, d3) in enumerate(CLASSES):
            s = b["s"][cls]
            lo, hi = lanes(b, cls, part)
            r1, y = b["r1"][cls], b["pr"][cls]
            for c in range(CORES):
                h = hperm[cls - 1, c] if cls else hbuf[:, c].reshape(HALF, FF)
                out = dot(h, vd[:, s + lo:s + hi]).astype(BF16).reshape(SIDE, SIDE, 16, hi - lo)
                for v in range(SIDE):
                    y[CORES * v + c, :, :, lo:hi] = out[v]
            for off in (2, 1, 3, 0):
                there, dev = along(d3, off)
                first = dev - core
                for flip in (0, 1):
                    there_core = core if flip == 0 else 1 - core
                    mine = y.at[CORES * there + there_core, :, :, lo:hi]
                    if off == 0 and flip == 0:
                        r1[there, core, :, :, lo:hi] = mine[...]
                        continue
                    links.copy(mine, r1.at[pos[d3], core, :, :, lo:hi], first + there_core,
                               ("back1", b["m"], cls), part, off)

    def back2(b, part):
        for cls, (d1, d2, d3) in enumerate(CLASSES):
            r1, r2 = b["r1"][cls], b["r2"][cls]
            lo, hi = lanes(b, cls, part)
            for off in (0, 1, 3, 2):
                chip = along(d3, (4 - off) % 4)[0]
                like = r1.at[0, :, :, :, lo:hi] if off else r1.at[0, 0, :, :, lo:hi]
                links.arrived(like, ("back1", b["m"], cls), part, off)
                for to in (2, 1, 3):
                    there, dev = along(d2, to)
                    links.copy(r1.at[chip, :, there, :, lo:hi], r2.at[pos[d2], chip, :, :, lo:hi], dev,
                               ("back2", b["m"], cls), part)
                r2[pos[d2], chip, :, :, lo:hi] = r1[chip, :, pos[d2], :, lo:hi]

    def weights(b, cls):
        d1, d2, d3 = CLASSES[cls]
        m = b["m"]
        route = routes[cls][pos[d2], m]
        gate = gates[cls][m]
        exp = iota((N_EXP, 1), 0).astype(F32)
        rank = rank_of(route, exp)
        value = jnp.zeros((N_EXP, COLUMN), F32)
        for j in range(TOP_K):
            value = jnp.where(route[j:j + 1] == exp, gate[j:j + 1], value)
        rank, value = rank.T.astype(BF16), value.T
        slot = iota((SLOTS, 1), 0)
        owner = pos[d1] * STRIDE[d1] + (slot >> 7) * STRIDE[d2] + ((slot >> 5) & 3) * STRIDE[d3] + ((slot >> 4) & 1)
        onehot = ones_where(iota((SLOTS, N_EXP), 1) == owner)
        col = iota((COLUMN, SLOTS), 1)
        keep = ((col >> 2) & 3) == (iota((COLUMN, SLOTS), 0) >> 5)
        keep = keep & (dot_nt(rank, onehot) == (col & 3).astype(F32))
        part1 = value.astype(BF16)
        rest = value - part1.astype(F32)
        part2 = rest.astype(BF16)
        part3 = (rest - part2.astype(F32)).astype(BF16)
        return jnp.concatenate(
            [jnp.where(keep, dot_nt(part, onehot), 0.0).astype(BF16) for part in (part3, part2, part1)], axis=0)

    def weigh(b):
        for cls in range(3):
            wts[cls] = weights(b, cls)

    def back3(b, part):
        for cls, (d1, d2, d3) in enumerate(CLASSES):
            lo, hi = lanes(b, cls, part)
            links.arrived(b["r2"][cls].at[0:3, :, :, :, lo:hi], ("back2", b["m"], cls), part)
            rows = b["r2"][cls][:, :, :, :, lo:hi].reshape(SLOTS, hi - lo)
            terms = dot(wts[cls], rows).reshape(3, COLUMN, hi - lo)
            sm, r3 = b["sm"][cls], b["r3"][cls]
            sm[:, :, lo:hi] = ((terms[0] + terms[1]) + terms[2]).reshape(SIDE, TOK, hi - lo)
            for off in (2, 1, 3):
                there, dev = along(d1, off)
                links.copy(sm.at[there, :, lo:hi], r3.at[pos[d1], :, lo:hi], dev, ("back3", b["m"], cls), part)
            r3[pos[d1], :, lo:hi] = sm[pos[d1], :, lo:hi]

    def finish(b, part, rows, out):
        for cls in range(3):
            s = b["s"][cls]
            lo, hi = lanes(b, cls, part)
            r3 = b["r3"][cls]
            links.arrived(r3.at[0:3, :, lo:hi], ("back3", b["m"], cls), part)
            total = (r3[0, :, lo:hi] + r3[1, :, lo:hi]) + (r3[2, :, lo:hi] + r3[3, :, lo:hi])
            out[:, s + lo:s + hi] = (rows[:, s + lo:s + hi].astype(F32) + total).astype(BF16)

    def drain(b, *names):
        for cls in range(3):
            likes = {"gather1": b["ag"][cls].at[0, 0:3], "gather2": b["ag"][cls].at[0:2], "relay2": b["ag"][cls].at[0],
                     "pick": b["pr"][cls].at[0:7], "back1": b["pr"][cls].at[0:7], "back2": b["r2"][cls].at[0:3],
                     "back3": b["r3"][cls].at[0:3]}
            for name in names:
                links.sent(likes[name], (name, b["m"], cls))

    a, b = batches
    write_meta()
    pl.semaphore_wait(barrier, len(peers))
    gather1(a, x_a)
    send_meta1()
    proj_step(0)
    proj_step(1)
    gather2(a)
    send_meta2()
    proj_step(2)
    for cls in range(3):
        pick(a, cls, 0)
    proj_step(3)
    proj_step(4)
    relay2(a)
    proj_step(5)
    for cls in range(3):
        links.arrived(routes[cls].at[0:3], ("meta2", cls))
        pick(a, cls, 1)
    proj_step(6)
    for cls in range(3):
        pick(a, cls, 3)
    proj_step(7)
    u_b[...] = (h_b[...].astype(F32) + proj_acc[...].astype(BF16).astype(F32)).astype(BF16)
    gather1(b, u_b)
    for cls in range(3):
        relayed(a, cls)
        pick(a, cls, 2)
    gather2(b)
    perms[0] = reorder(0, 1)
    perms[1] = reorder(0, 2)
    perms[2] = reorder(1, 0)
    perms[3] = reorder(2, 0)
    for cls in range(3):
        pick(b, cls, 0)
    qkv_step(0)
    relay2(b)
    for cls in range(3):
        pick(b, cls, 1)
        pick(b, cls, 3)
    qkv_step(1)
    for cls in range(3):
        relayed(b, cls)
        pick(b, cls, 2)
    for c in w_copies:
        c.wait()
    experts(a)
    align(a)
    back1(a, 0)
    back1(a, 1)
    experts(b)
    back2(a, 0)
    align(b)
    back1(b, 0)
    back2(a, 1)
    back1(b, 1)
    weigh(a)
    qkv_step(2)
    back3(a, 0)
    back2(b, 0)
    qkv_step(3)
    back3(a, 1)
    back2(b, 1)
    weigh(b)
    for i in range(4, n_wq):
        qkv_step(i)
    finish(a, 0, x_a, out_a)
    finish(a, 1, x_a, out_a)
    for cls in range(3):
        links.sent(meta[cls].at[0:3], ("meta1", cls))
        links.sent(routes[cls].at[0:3], ("meta2", cls))
    drain(a, "gather1", "gather2", "relay2", "pick", "back1", "back2", "back3")
    drain(b, "gather1", "gather2", "relay2", "pick", "back1")
    back3(b, 0)
    back3(b, 1)
    finish(b, 0, u_b, out_b)
    drain(b, "back2")
    finish(b, 1, u_b, out_b)
    drain(b, "back3")


def deliver(*refs):
    n = (len(refs) - 1) // 2
    ops = [pltpu.make_async_copy(refs[i], refs[n + i], refs[-1].at[i]) for i in range(n)]
    for op in ops:
        op.start()
    for op in ops:
        op.wait()


def solution(mesh):
    def local_step(x_a, route_a, gate_a, h_b, attn_b, route_b, gate_b, w_qkv, w_o, w_gate, w_up, w_down):
        vmem = pl.BlockSpec(memory_space=pltpu.VMEM)
        hbm = pl.BlockSpec(memory_space=pl.ANY)
        scratch = []
        for m in range(2):
            for shape, dtype in (
                (lambda w: (SIDE, SIDE, TOK, w), BF16),
                (lambda w: (SIDE, SIDE, CORES, 16, w), BF16),
                (lambda w: (SIDE * CORES, SIDE, 16, w), BF16),
                (lambda w: (SIDE, CORES, SIDE, 16, w), BF16),
                (lambda w: (SIDE, SIDE, CORES, 16, w), BF16),
                (lambda w: (SIDE, TOK, w), F32),
                (lambda w: (SIDE, TOK, w), F32),
            ):
                scratch += [pltpu.VMEM(shape(w), dtype) for w in WIDTHS[m]]
        scratch += [pltpu.VMEM((SIDE, 2, TOP_K, COLUMN), F32)] * 3
        scratch += [pltpu.VMEM((SIDE, 2, TOP_K, COLUMN), F32)] * 3
        scratch += [pltpu.VMEM((2, TOP_K, COLUMN), F32)] * 3
        scratch += [
            pltpu.VMEM((SIDE, CORES, 64, D), BF16),
            pltpu.VMEM((SIDE, CORES, 64, FF), BF16),
            pltpu.VMEM((2, CORES, HALF, FF), BF16),
            pltpu.VMEM((3, 3 * COLUMN, SLOTS), BF16),
            pltpu.VMEM((4, HALF, HALF), BF16),
            pltpu.VMEM((TOK, D), F32),
            pltpu.VMEM((TOK, QKV), F32),
            pltpu.VMEM((TOK, D), BF16),
            pltpu.VMEM((D, FF), BF16),
            pltpu.VMEM((D, FF), BF16),
            pltpu.VMEM((FF, D), BF16),
            pltpu.VMEM((2, WO_CHUNK, D), BF16),
            pltpu.VMEM((2, WQ_CHUNK, QKV), BF16),
            pltpu.SemaphoreType.DMA((N_PHASES,)),
            pltpu.SemaphoreType.DMA((N_GROUPS,)),
            pltpu.SemaphoreType.DMA((3,)),
            pltpu.SemaphoreType.DMA((2,)),
            pltpu.SemaphoreType.DMA((2,)),
        ]
        outs = tuple(jax.ShapeDtypeStruct((TOK, n), BF16) for n in (D, D, QKV))
        results = pl.pallas_call(
            kernel,
            out_shape=outs,
            in_specs=[vmem] * 7 + [hbm] * 5,
            out_specs=(vmem,) * 3,
            scratch_shapes=scratch,
            name="moe_pair",
            compiler_params=pltpu.CompilerParams(
                collective_id=0, has_side_effects=True, vmem_limit_bytes=64 * 2**20 - 2**16),
        )(x_a, h_b, attn_b, route_a.T, route_b.T, gate_a.T, gate_b.T, w_qkv, w_o, w_gate, w_up, w_down)
        return pl.pallas_call(
            deliver,
            out_shape=outs,
            in_specs=[hbm] * 3,
            out_specs=(vmem,) * 3,
            scratch_shapes=[pltpu.SemaphoreType.DMA((3,))],
            name="deliver",
        )(*results)

    row_spec = P(("dp", "ep"), None)
    full_spec = P(None, None)
    expert_spec = P("ep", None, None)
    return jax.shard_map(
        local_step,
        mesh=mesh,
        in_specs=(row_spec,) * 7 + (full_spec, full_spec) + (expert_spec,) * 3,
        out_specs=(row_spec, row_spec, row_spec),
        check_vma=False,
    )
```

```python
import jax
import jax.numpy as jnp
from jax import lax
from jax.experimental import pallas as pl
from jax.experimental.pallas import tpu as pltpu
from jax.sharding import PartitionSpec as P

MESH = pl.DeviceIdType.MESH
BF16 = jnp.bfloat16
F32 = jnp.float32

SIDE = 4
CORES = 2
TOK = 32
CAP = 4
TOP_K = 8
D = 2048
N_EXP = 128
FF = 768
ATT = 4096
QKV = 5120
SLOTS = N_EXP * CAP
CLASSES = ((0, 1, 2), (1, 2, 0), (2, 0, 1))
WIDTHS = ((768, 640, 640), (640, 768, 640))
STARTS = ((0, 768, 1408), (0, 640, 1408))
STRIDE = (32, 8, 2)
UNUSED = 8.0
WO_CHUNK = 512
WQ_CHUNK = 256
HALF = SLOTS // 2
COLUMN = SIDE * TOK


def iota(shape, dim):
    return lax.broadcasted_iota(jnp.int32, shape, dim)


def ones_where(cond):
    return jnp.where(cond, 1.0, 0.0).astype(BF16)


def dot(a, b):
    return jnp.dot(a, b, preferred_element_type=F32)


def dot_nt(a, b):
    return lax.dot_general(a, b, (((1,), (1,)), ((), ())), preferred_element_type=F32)


def reorder(to_cls, from_cls):
    row = iota((HALF, 1), 0)
    d1, d2, d3 = CLASSES[to_cls]
    coords = {d3: row >> 6, d2: (row >> 4) & 3, d1: (row >> 2) & 3}
    d1, d2, d3 = CLASSES[from_cls]
    want = (coords[d3] << 6) | (coords[d2] << 4) | (coords[d1] << 2) | (row & 3)
    return ones_where(iota((HALF, HALF), 1) == want)


class Links:
    def __init__(self, send, recv, other):
        self.send, self.recv, self.other, self.sends, self.recvs = send, recv, other, {}, {}

    def _op(self, src, dst, device, phase, group):
        i = self.sends.setdefault(phase, len(self.sends))
        j = self.recvs.setdefault(group, len(self.recvs))
        return pltpu.make_async_remote_copy(
            src_ref=src, dst_ref=dst, send_sem=self.send.at[i], recv_sem=self.recv.at[j],
            device_id={"ep": device}, device_id_type=MESH)

    def copy(self, src, dst, device, phase, *rest):
        self._op(src, dst, device, phase, phase + rest).start()

    def arrived(self, like, phase, *rest):
        self._op(like, like, self.other, phase, phase + rest).wait_recv()

    def sent(self, like, phase):
        self._op(like, like, self.other, phase, next(g for g in self.recvs if g[:len(phase)] == phase)).wait_send()


N_PHASES = 6 + 2 * 21
N_GROUPS = 6 + 2 * (3 + 3 + 3 + 3 + 24 + 6 + 6)
FIRST = 384


def kernel(*refs):
    it = iter(refs)
    take = lambda n: [next(it) for _ in range(n)]
    x_a, h_b, attn, route_a, route_b, gate_a, gate_b = take(7)
    w_qkv, w_o, w_gate, w_up, w_down = take(5)
    out_a, out_b, qkv_out = take(3)
    batches = []
    for m in range(2):
        b = {"m": m, "w": WIDTHS[m], "s": STARTS[m]}
        for name in ("ag", "ps", "pr", "r1", "r2", "sm", "r3"):
            b[name] = take(3)
        batches.append(b)
    meta, routes, gates = take(3), take(3), take(3)
    xbuf, hbuf, hperm, wts, perms, proj_acc, qkv_acc, u_b = take(8)
    vg, vu, vd, wo_buf, wq_buf = take(5)
    send_sem, recv_sem, w_sem, wo_sem, wq_sem = take(5)

    me = lax.axis_index("ep")
    core = lax.rem(me, 2)
    pos = [lax.rem(me // 32, 4), lax.rem(me // 8, 4), lax.rem(me // 2, 4)]
    links = Links(send_sem, recv_sem, me + 1 - 2 * core)

    def along(dim, off):
        there = lax.rem(pos[dim] + off, 4)
        return there, me + (there - pos[dim]) * STRIDE[dim]

    peers = []
    for dim in range(3):
        for off in (1, 2, 3):
            _, dev = along(dim, off)
            peers += [dev, dev + 1 - 2 * core]
    peers.append(me + 1 - 2 * core)
    barrier = pltpu.get_barrier_semaphore()
    for dev in peers:
        pl.semaphore_signal(barrier, inc=1, device_id={"ep": dev}, device_id_type=MESH)

    w_copies = [pltpu.make_async_copy(src.at[0], dst, w_sem.at[i])
                for i, (src, dst) in enumerate(((w_gate, vg), (w_up, vu), (w_down, vd)))]
    n_wo, n_wq = ATT // WO_CHUNK, D // WQ_CHUNK

    def wo_copy(i):
        return pltpu.make_async_copy(w_o.at[pl.ds(i * WO_CHUNK, WO_CHUNK)], wo_buf.at[i % 2], wo_sem.at[i % 2])

    def wq_copy(i):
        return pltpu.make_async_copy(w_qkv.at[pl.ds(i * WQ_CHUNK, WQ_CHUNK)], wq_buf.at[i % 2], wq_sem.at[i % 2])

    wo_copy(0).start()
    wo_copy(1).start()

    def proj_step(i):
        wo_copy(i).wait()
        part = dot(attn[:, i * WO_CHUNK:(i + 1) * WO_CHUNK], wo_buf[i % 2])
        proj_acc[...] = part if i == 0 else proj_acc[...] + part
        if i + 2 < n_wo:
            wo_copy(i + 2).start()

    def qkv_step(i):
        wq_copy(i).wait()
        part = dot(h_b[:, i * WQ_CHUNK:(i + 1) * WQ_CHUNK], wq_buf[i % 2])
        if i == n_wq - 1:
            qkv_out[...] = (qkv_acc[...] + part).astype(BF16)
        else:
            qkv_acc[...] = part if i == 0 else qkv_acc[...] + part
        if i + 2 < n_wq:
            wq_copy(i + 2).start()

    earlier = ones_where((iota((COLUMN, COLUMN), 0) < iota((COLUMN, COLUMN), 1))
                         & (iota((COLUMN, COLUMN), 0) >> 5 == iota((COLUMN, COLUMN), 1) >> 5))

    def rank_of(route, expert):
        hit = route[0:1] == expert
        for j in range(1, TOP_K):
            hit = hit | (route[j:j + 1] == expert)
        rank = dot(ones_where(hit), earlier)
        return jnp.where(hit, rank, UNUSED)

    def write_meta():
        for cls, (d1, d2, d3) in enumerate(CLASSES):
            for i, (a, b) in enumerate(((route_a, route_b), (gate_a, gate_b))):
                meta[cls][pos[d1], i] = jnp.zeros((TOP_K, N_EXP), F32)
                meta[cls][pos[d1], i, :, 0:TOK] = a[...].astype(F32)
                meta[cls][pos[d1], i, :, TOK:2 * TOK] = b[...].astype(F32)

    def send_meta1():
        for cls, (d1, d2, d3) in enumerate(CLASSES):
            mine = meta[cls].at[pos[d1]]
            for off in (2, 1, 3):
                links.copy(mine, mine, along(d1, off)[1], ("meta1", cls))

    def send_meta2():
        lane = iota((TOP_K, COLUMN), 1) >> 5
        for cls, (d1, d2, d3) in enumerate(CLASSES):
            links.arrived(meta[cls].at[0:3], ("meta1", cls))
            for i, dst in ((0, routes[cls].at[pos[d2]]), (1, gates[cls])):
                for m in range(2):
                    packed = jnp.zeros((TOP_K, COLUMN), F32)
                    for v in range(SIDE):
                        shift = (TOK * (v - m)) % COLUMN
                        piece = meta[cls][v, i]
                        packed = jnp.where(lane == v, pltpu.roll(piece, shift, 1) if shift else piece, packed)
                    dst[m] = packed
            mine = routes[cls].at[pos[d2]]
            for off in (2, 1, 3):
                links.copy(mine, mine, along(d2, off)[1], ("meta2", cls))

    def gather1(b, rows):
        for cls, (d1, d2, d3) in enumerate(CLASSES):
            w, s = b["w"][cls], b["s"][cls]
            for off in (2, 1, 3):
                links.copy(rows.at[:, s:s + w], b["ag"][cls].at[pos[d2], pos[d1]], along(d1, off)[1],
                           ("gather1", b["m"], cls))
        for cls, (d1, d2, d3) in enumerate(CLASSES):
            w, s = b["w"][cls], b["s"][cls]
            b["ag"][cls][pos[d2], pos[d1]] = rows[:, s:s + w]

    def gather2(b):
        for cls, (d1, d2, d3) in enumerate(CLASSES):
            ag = b["ag"][cls]
            links.arrived(ag.at[0, 0:3], ("gather1", b["m"], cls))
            mine = ag.at[pos[d2]]
            for off in (1, 3):
                links.copy(mine, mine, along(d2, off)[1], ("gather2", b["m"], cls))

    def relay2(b):
        for cls, (d1, d2, d3) in enumerate(CLASSES):
            ag = b["ag"][cls]
            links.arrived(ag.at[0:2], ("gather2", b["m"], cls))
            for off, half in ((1, 0), (3, 2)):
                got = ag.at[along(d2, 4 - off)[0], half:half + 2]
                links.copy(got, got, along(d2, off)[1], ("relay2", b["m"], cls))

    def relayed(b, cls):
        links.arrived(b["ag"][cls].at[0], ("relay2", b["m"], cls))

    def pick(b, cls, off2):
        d1, d2, d3 = CLASSES[cls]
        w = b["w"][cls]
        block = along(d2, off2)[0]
        exp = iota((SIDE * CORES, 1), 0)
        exp = me - pos[d3] * STRIDE[d3] - core + (exp >> 1) * STRIDE[d3] + (exp & 1)
        rank = rank_of(routes[cls][block, b["m"]], exp.astype(F32))
        rank = jnp.concatenate([jnp.broadcast_to(rank[e:e + 1], (16, COLUMN)) for e in range(SIDE * CORES)], axis=0)
        slot = iota((COLUMN, 1), 0)
        mask = ((slot >> 2) & 3) == (iota((COLUMN, COLUMN), 1) >> 5)
        choice = ones_where(mask & (rank == (slot & 3).astype(F32)))
        got = dot(choice, b["ag"][cls][block].reshape(COLUMN, w)).astype(BF16)
        ps, pr = b["ps"][cls], b["pr"][cls]
        ps[block] = got.reshape(SIDE, CORES, 16, w)
        for off in (2, 1, 3, 0):
            there, dev = along(d3, off)
            first = dev - core
            for flip in (0, 1):
                there_core = core if flip == 0 else 1 - core
                if off == 0 and flip == 0:
                    pr[CORES * there + core, block] = ps[block, there, core]
                    continue
                links.copy(ps.at[block, there, there_core], pr.at[CORES * pos[d3] + core, block], first + there_core,
                           ("pick", b["m"], cls))

    def received(b):
        for cls in range(3):
            s, w = b["s"][cls], b["w"][cls]
            pr = b["pr"][cls]
            links.arrived(pr.at[0:7], ("pick", b["m"], cls))
            for c in range(CORES):
                rows = jnp.concatenate([pr[CORES * v + c].reshape(64, w) for v in range(SIDE)], axis=0)
                if cls:
                    rows = dot(perms[cls - 1], rows).astype(BF16)
                xbuf[:, c, :, s:s + w] = rows.reshape(SIDE, 64, w)

    def hidden(first, last):
        @pl.loop(first, last)
        def _(i):
            cols = pl.ds(pl.multiple_of(i * 256, 256), 256)
            x = xbuf[...].reshape(SLOTS, D)
            g = dot(x, vg[:, cols])
            u = dot(x, vu[:, cols])
            h = (g * (1.0 / (1.0 + jnp.exp(-g))) * u).astype(BF16)
            hbuf[:, :, :, cols] = h.reshape(SIDE, CORES, 64, 256)

    def lanes(b, cls, part):
        return (0, FIRST) if part == 0 else (FIRST, b["w"][cls])

    def align(b):
        for cls in (1, 2):
            for c in range(CORES):
                hperm[cls - 1, c] = dot(perms[cls + 1], hbuf[:, c].reshape(HALF, FF)).astype(BF16)

    def back1(b, part):
        for cls, (d1, d2, d3) in enumerate(CLASSES):
            s = b["s"][cls]
            lo, hi = lanes(b, cls, part)
            r1, y = b["r1"][cls], b["pr"][cls]
            for c in range(CORES):
                h = hperm[cls - 1, c] if cls else hbuf[:, c].reshape(HALF, FF)
                out = dot(h, vd[:, s + lo:s + hi]).astype(BF16).reshape(SIDE, SIDE, 16, hi - lo)
                for v in range(SIDE):
                    y[CORES * v + c, :, :, lo:hi] = out[v]
            for off in (2, 1, 3, 0):
                there, dev = along(d3, off)
                first = dev - core
                for flip in (0, 1):
                    there_core = core if flip == 0 else 1 - core
                    mine = y.at[CORES * there + there_core, :, :, lo:hi]
                    if off == 0 and flip == 0:
                        r1[there, core, :, :, lo:hi] = mine[...]
                        continue
                    links.copy(mine, r1.at[pos[d3], core, :, :, lo:hi], first + there_core,
                               ("back1", b["m"], cls), part, off)

    def back2(b, part):
        for cls, (d1, d2, d3) in enumerate(CLASSES):
            r1, r2 = b["r1"][cls], b["r2"][cls]
            lo, hi = lanes(b, cls, part)
            for off in (0, 1, 3, 2):
                chip = along(d3, (4 - off) % 4)[0]
                like = r1.at[0, :, :, :, lo:hi] if off else r1.at[0, 0, :, :, lo:hi]
                links.arrived(like, ("back1", b["m"], cls), part, off)
                for to in (2, 1, 3):
                    there, dev = along(d2, to)
                    links.copy(r1.at[chip, :, there, :, lo:hi], r2.at[pos[d2], chip, :, :, lo:hi], dev,
                               ("back2", b["m"], cls), part)
                r2[pos[d2], chip, :, :, lo:hi] = r1[chip, :, pos[d2], :, lo:hi]

    def weights(b, cls):
        d1, d2, d3 = CLASSES[cls]
        m = b["m"]
        route = routes[cls][pos[d2], m]
        gate = gates[cls][m]
        exp = iota((N_EXP, 1), 0).astype(F32)
        rank = rank_of(route, exp)
        value = jnp.zeros((N_EXP, COLUMN), F32)
        for j in range(TOP_K):
            value = jnp.where(route[j:j + 1] == exp, gate[j:j + 1], value)
        rank, value = rank.T.astype(BF16), value.T
        slot = iota((SLOTS, 1), 0)
        owner = pos[d1] * STRIDE[d1] + (slot >> 7) * STRIDE[d2] + ((slot >> 5) & 3) * STRIDE[d3] + ((slot >> 4) & 1)
        onehot = ones_where(iota((SLOTS, N_EXP), 1) == owner)
        col = iota((COLUMN, SLOTS), 1)
        keep = ((col >> 2) & 3) == (iota((COLUMN, SLOTS), 0) >> 5)
        keep = keep & (dot_nt(rank, onehot) == (col & 3).astype(F32))
        part1 = value.astype(BF16)
        rest = value - part1.astype(F32)
        part2 = rest.astype(BF16)
        part3 = (rest - part2.astype(F32)).astype(BF16)
        return jnp.concatenate(
            [jnp.where(keep, dot_nt(part, onehot), 0.0).astype(BF16) for part in (part3, part2, part1)], axis=0)

    def weigh(b):
        for cls in range(3):
            wts[cls] = weights(b, cls)

    def back3(b, part):
        for cls, (d1, d2, d3) in enumerate(CLASSES):
            lo, hi = lanes(b, cls, part)
            links.arrived(b["r2"][cls].at[0:3, :, :, :, lo:hi], ("back2", b["m"], cls), part)
            rows = b["r2"][cls][:, :, :, :, lo:hi].reshape(SLOTS, hi - lo)
            terms = dot(wts[cls], rows).reshape(3, COLUMN, hi - lo)
            sm, r3 = b["sm"][cls], b["r3"][cls]
            sm[:, :, lo:hi] = ((terms[0] + terms[1]) + terms[2]).reshape(SIDE, TOK, hi - lo)
            for off in (2, 1, 3):
                there, dev = along(d1, off)
                links.copy(sm.at[there, :, lo:hi], r3.at[pos[d1], :, lo:hi], dev, ("back3", b["m"], cls), part)
            r3[pos[d1], :, lo:hi] = sm[pos[d1], :, lo:hi]

    def finish(b, part, rows, out):
        for cls in range(3):
            s = b["s"][cls]
            lo, hi = lanes(b, cls, part)
            r3 = b["r3"][cls]
            links.arrived(r3.at[0:3, :, lo:hi], ("back3", b["m"], cls), part)
            total = (r3[0, :, lo:hi] + r3[1, :, lo:hi]) + (r3[2, :, lo:hi] + r3[3, :, lo:hi])
            out[:, s + lo:s + hi] = (rows[:, s + lo:s + hi].astype(F32) + total).astype(BF16)

    def drain(b, *names):
        for cls in range(3):
            likes = {"gather1": b["ag"][cls].at[0, 0:3], "gather2": b["ag"][cls].at[0:2], "relay2": b["ag"][cls].at[0],
                     "pick": b["pr"][cls].at[0:7], "back1": b["pr"][cls].at[0:7], "back2": b["r2"][cls].at[0:3],
                     "back3": b["r3"][cls].at[0:3]}
            for name in names:
                links.sent(likes[name], (name, b["m"], cls))

    a, b = batches
    write_meta()
    pl.semaphore_wait(barrier, len(peers))
    gather1(a, x_a)
    send_meta1()
    for i in range(4):
        proj_step(i)
    gather2(a)
    send_meta2()
    for i in range(4, n_wo):
        proj_step(i)
    u_b[...] = (h_b[...].astype(F32) + proj_acc[...].astype(BF16).astype(F32)).astype(BF16)
    gather1(b, u_b)
    for c in w_copies:
        c.start()
    wq_copy(0).start()
    wq_copy(1).start()
    for cls in range(3):
        pick(a, cls, 0)
    perms[0] = reorder(0, 1)
    perms[1] = reorder(0, 2)
    relay2(a)
    for cls in range(3):
        links.arrived(routes[cls].at[0:3], ("meta2", cls))
        pick(a, cls, 1)
        pick(a, cls, 3)
    gather2(b)
    for cls in range(3):
        relayed(a, cls)
        pick(a, cls, 2)
    for cls in range(3):
        pick(b, cls, 0)
    perms[2] = reorder(1, 0)
    perms[3] = reorder(2, 0)
    qkv_step(0)
    relay2(b)
    for cls in range(3):
        pick(b, cls, 1)
        pick(b, cls, 3)
    for c in w_copies:
        c.wait()
    received(a)
    hidden(0, 2)
    for cls in range(3):
        relayed(b, cls)
        pick(b, cls, 2)
    hidden(2, 3)
    align(a)
    back1(a, 0)
    back1(a, 1)
    qkv_step(1)
    qkv_step(2)
    received(b)
    hidden(0, 3)
    back2(a, 0)
    align(b)
    back1(b, 0)
    back2(a, 1)
    back1(b, 1)
    weigh(a)
    qkv_step(3)
    back2(b, 0)
    back3(a, 0)
    back2(b, 1)
    back3(a, 1)
    weigh(b)
    for i in range(4, n_wq):
        qkv_step(i)
    finish(a, 0, x_a, out_a)
    finish(a, 1, x_a, out_a)
    for cls in range(3):
        links.sent(meta[cls].at[0:3], ("meta1", cls))
        links.sent(routes[cls].at[0:3], ("meta2", cls))
    drain(a, "gather1", "gather2", "relay2", "pick", "back1", "back2", "back3")
    drain(b, "gather1", "gather2", "relay2", "pick", "back1")
    back3(b, 0)
    back3(b, 1)
    finish(b, 0, u_b, out_b)
    drain(b, "back2")
    finish(b, 1, u_b, out_b)
    drain(b, "back3")


def deliver(*refs):
    n = (len(refs) - 1) // 2
    ops = [pltpu.make_async_copy(refs[i], refs[n + i], refs[-1].at[i]) for i in range(n)]
    for op in ops:
        op.start()
    for op in ops:
        op.wait()


def solution(mesh):
    def local_step(x_a, route_a, gate_a, h_b, attn_b, route_b, gate_b, w_qkv, w_o, w_gate, w_up, w_down):
        vmem = pl.BlockSpec(memory_space=pltpu.VMEM)
        hbm = pl.BlockSpec(memory_space=pl.ANY)
        scratch = []
        for m in range(2):
            for shape, dtype in (
                (lambda w: (SIDE, SIDE, TOK, w), BF16),
                (lambda w: (SIDE, SIDE, CORES, 16, w), BF16),
                (lambda w: (SIDE * CORES, SIDE, 16, w), BF16),
                (lambda w: (SIDE, CORES, SIDE, 16, w), BF16),
                (lambda w: (SIDE, SIDE, CORES, 16, w), BF16),
                (lambda w: (SIDE, TOK, w), F32),
                (lambda w: (SIDE, TOK, w), F32),
            ):
                scratch += [pltpu.VMEM(shape(w), dtype) for w in WIDTHS[m]]
        scratch += [pltpu.VMEM((SIDE, 2, TOP_K, COLUMN), F32)] * 3
        scratch += [pltpu.VMEM((SIDE, 2, TOP_K, COLUMN), F32)] * 3
        scratch += [pltpu.VMEM((2, TOP_K, COLUMN), F32)] * 3
        scratch += [
            pltpu.VMEM((SIDE, CORES, 64, D), BF16),
            pltpu.VMEM((SIDE, CORES, 64, FF), BF16),
            pltpu.VMEM((2, CORES, HALF, FF), BF16),
            pltpu.VMEM((3, 3 * COLUMN, SLOTS), BF16),
            pltpu.VMEM((4, HALF, HALF), BF16),
            pltpu.VMEM((TOK, D), F32),
            pltpu.VMEM((TOK, QKV), F32),
            pltpu.VMEM((TOK, D), BF16),
            pltpu.VMEM((D, FF), BF16),
            pltpu.VMEM((D, FF), BF16),
            pltpu.VMEM((FF, D), BF16),
            pltpu.VMEM((2, WO_CHUNK, D), BF16),
            pltpu.VMEM((2, WQ_CHUNK, QKV), BF16),
            pltpu.SemaphoreType.DMA((N_PHASES,)),
            pltpu.SemaphoreType.DMA((N_GROUPS,)),
            pltpu.SemaphoreType.DMA((3,)),
            pltpu.SemaphoreType.DMA((2,)),
            pltpu.SemaphoreType.DMA((2,)),
        ]
        outs = tuple(jax.ShapeDtypeStruct((TOK, n), BF16) for n in (D, D, QKV))
        results = pl.pallas_call(
            kernel,
            out_shape=outs,
            in_specs=[vmem] * 7 + [hbm] * 5,
            out_specs=(vmem,) * 3,
            scratch_shapes=scratch,
            name="moe_pair",
            compiler_params=pltpu.CompilerParams(
                collective_id=0, has_side_effects=True, vmem_limit_bytes=64 * 2**20 - 2**16),
        )(x_a, h_b, attn_b, route_a.T, route_b.T, gate_a.T, gate_b.T, w_qkv, w_o, w_gate, w_up, w_down)
        return pl.pallas_call(
            deliver,
            out_shape=outs,
            in_specs=[hbm] * 3,
            out_specs=(vmem,) * 3,
            scratch_shapes=[pltpu.SemaphoreType.DMA((3,))],
            name="deliver",
        )(*results)

    row_spec = P(("dp", "ep"), None)
    full_spec = P(None, None)
    expert_spec = P("ep", None, None)
    return jax.shard_map(
        local_step,
        mesh=mesh,
        in_specs=(row_spec,) * 7 + (full_spec, full_spec) + (expert_spec,) * 3,
        out_specs=(row_spec, row_spec, row_spec),
        check_vma=False,
    )
```

```python
import jax
import jax.numpy as jnp
from jax import lax
from jax.experimental import pallas as pl
from jax.experimental.pallas import tpu as pltpu
from jax.sharding import PartitionSpec as P

MESH = pl.DeviceIdType.MESH
BF16 = jnp.bfloat16
F32 = jnp.float32

SIDE = 4
CORES = 2
TOK = 32
CAP = 4
TOP_K = 8
D = 2048
N_EXP = 128
FF = 768
ATT = 4096
QKV = 5120
SLOTS = N_EXP * CAP
CLASSES = ((0, 1, 2), (1, 2, 0), (2, 0, 1))
WIDTHS = ((768, 640, 640), (640, 768, 640))
STARTS = ((0, 768, 1408), (0, 640, 1408))
STRIDE = (32, 8, 2)
UNUSED = 8.0
WO_CHUNK = 512
WQ_CHUNK = 256
HALF = SLOTS // 2
COLUMN = SIDE * TOK


def iota(shape, dim):
    return lax.broadcasted_iota(jnp.int32, shape, dim)


def ones_where(cond):
    return jnp.where(cond, 1.0, 0.0).astype(BF16)


def dot(a, b):
    return jnp.dot(a, b, preferred_element_type=F32)


def dot_nt(a, b):
    return lax.dot_general(a, b, (((1,), (1,)), ((), ())), preferred_element_type=F32)


def reorder(to_cls, from_cls):
    row = iota((HALF, 1), 0)
    d1, d2, d3 = CLASSES[to_cls]
    coords = {d3: row >> 6, d2: (row >> 4) & 3, d1: (row >> 2) & 3}
    d1, d2, d3 = CLASSES[from_cls]
    want = (coords[d3] << 6) | (coords[d2] << 4) | (coords[d1] << 2) | (row & 3)
    return ones_where(iota((HALF, HALF), 1) == want)


class Links:
    def __init__(self, send, recv, other):
        self.send, self.recv, self.other, self.sends, self.recvs = send, recv, other, {}, {}

    def _op(self, src, dst, device, phase, group):
        i = self.sends.setdefault(phase, len(self.sends))
        j = self.recvs.setdefault(group, len(self.recvs))
        return pltpu.make_async_remote_copy(
            src_ref=src, dst_ref=dst, send_sem=self.send.at[i], recv_sem=self.recv.at[j],
            device_id={"ep": device}, device_id_type=MESH)

    def copy(self, src, dst, device, phase, *rest):
        self._op(src, dst, device, phase, phase + rest).start()

    def arrived(self, like, phase, *rest):
        self._op(like, like, self.other, phase, phase + rest).wait_recv()

    def sent(self, like, phase):
        self._op(like, like, self.other, phase, next(g for g in self.recvs if g[:len(phase)] == phase)).wait_send()


N_PHASES = 6 + 2 * 21
N_GROUPS = 6 + 2 * (3 + 3 + 3 + 3 + 24 + 6 + 6)
FIRST = 384


def kernel(*refs):
    it = iter(refs)
    take = lambda n: [next(it) for _ in range(n)]
    x_a, h_b, attn, route_a, route_b, gate_a, gate_b = take(7)
    w_qkv, w_o, w_gate, w_up, w_down = take(5)
    out_a, out_b, qkv_out = take(3)
    batches = []
    for m in range(2):
        b = {"m": m, "w": WIDTHS[m], "s": STARTS[m]}
        for name in ("ag", "ps", "pr", "r1", "r2", "sm", "r3"):
            b[name] = take(3)
        batches.append(b)
    meta, routes, gates = take(3), take(3), take(3)
    xbuf, hbuf, hperm, wts, perms, proj_acc, qkv_acc, u_b = take(8)
    vg, vu, vd, wo_buf, wq_buf = take(5)
    send_sem, recv_sem, w_sem, wo_sem, wq_sem = take(5)

    me = lax.axis_index("ep")
    core = lax.rem(me, 2)
    pos = [lax.rem(me // 32, 4), lax.rem(me // 8, 4), lax.rem(me // 2, 4)]
    links = Links(send_sem, recv_sem, me + 1 - 2 * core)

    def along(dim, off):
        there = lax.rem(pos[dim] + off, 4)
        return there, me + (there - pos[dim]) * STRIDE[dim]

    peers = []
    for dim in range(3):
        for off in (1, 2, 3):
            _, dev = along(dim, off)
            peers += [dev, dev + 1 - 2 * core]
    peers.append(me + 1 - 2 * core)
    barrier = pltpu.get_barrier_semaphore()
    for dev in peers:
        pl.semaphore_signal(barrier, inc=1, device_id={"ep": dev}, device_id_type=MESH)

    w_copies = [pltpu.make_async_copy(src.at[0], dst, w_sem.at[i])
                for i, (src, dst) in enumerate(((w_gate, vg), (w_up, vu), (w_down, vd)))]
    n_wo, n_wq = ATT // WO_CHUNK, D // WQ_CHUNK

    def wo_copy(i):
        return pltpu.make_async_copy(w_o.at[pl.ds(i * WO_CHUNK, WO_CHUNK)], wo_buf.at[i % 2], wo_sem.at[i % 2])

    def wq_copy(i):
        return pltpu.make_async_copy(w_qkv.at[pl.ds(i * WQ_CHUNK, WQ_CHUNK)], wq_buf.at[i % 2], wq_sem.at[i % 2])

    wo_copy(0).start()
    wo_copy(1).start()

    def proj_step(i):
        wo_copy(i).wait()
        part = dot(attn[:, i * WO_CHUNK:(i + 1) * WO_CHUNK], wo_buf[i % 2])
        proj_acc[...] = part if i == 0 else proj_acc[...] + part
        if i + 2 < n_wo:
            wo_copy(i + 2).start()

    def qkv_step(i):
        wq_copy(i).wait()
        part = dot(h_b[:, i * WQ_CHUNK:(i + 1) * WQ_CHUNK], wq_buf[i % 2])
        if i == n_wq - 1:
            qkv_out[...] = (qkv_acc[...] + part).astype(BF16)
        else:
            qkv_acc[...] = part if i == 0 else qkv_acc[...] + part
        if i + 2 < n_wq:
            wq_copy(i + 2).start()

    earlier = ones_where((iota((COLUMN, COLUMN), 0) < iota((COLUMN, COLUMN), 1))
                         & (iota((COLUMN, COLUMN), 0) >> 5 == iota((COLUMN, COLUMN), 1) >> 5))

    def rank_of(route, expert):
        hit = route[0:1] == expert
        for j in range(1, TOP_K):
            hit = hit | (route[j:j + 1] == expert)
        rank = dot(ones_where(hit), earlier)
        return jnp.where(hit, rank, UNUSED)

    def write_meta():
        for cls, (d1, d2, d3) in enumerate(CLASSES):
            for i, (a, b) in enumerate(((route_a, route_b), (gate_a, gate_b))):
                meta[cls][pos[d1], i] = jnp.zeros((TOP_K, N_EXP), F32)
                meta[cls][pos[d1], i, :, 0:TOK] = a[...].astype(F32)
                meta[cls][pos[d1], i, :, TOK:2 * TOK] = b[...].astype(F32)

    def send_meta1():
        for cls, (d1, d2, d3) in enumerate(CLASSES):
            mine = meta[cls].at[pos[d1]]
            for off in (2, 1, 3):
                links.copy(mine, mine, along(d1, off)[1], ("meta1", cls))

    def send_meta2():
        lane = iota((TOP_K, COLUMN), 1) >> 5
        for cls, (d1, d2, d3) in enumerate(CLASSES):
            links.arrived(meta[cls].at[0:3], ("meta1", cls))
            for i, dst in ((0, routes[cls].at[pos[d2]]), (1, gates[cls])):
                for m in range(2):
                    packed = jnp.zeros((TOP_K, COLUMN), F32)
                    for v in range(SIDE):
                        shift = (TOK * (v - m)) % COLUMN
                        piece = meta[cls][v, i]
                        packed = jnp.where(lane == v, pltpu.roll(piece, shift, 1) if shift else piece, packed)
                    dst[m] = packed
            mine = routes[cls].at[pos[d2]]
            for off in (2, 1, 3):
                links.copy(mine, mine, along(d2, off)[1], ("meta2", cls))

    def gather1(b, rows):
        for cls, (d1, d2, d3) in enumerate(CLASSES):
            w, s = b["w"][cls], b["s"][cls]
            for off in (2, 1, 3):
                links.copy(rows.at[:, s:s + w], b["ag"][cls].at[pos[d2], pos[d1]], along(d1, off)[1],
                           ("gather1", b["m"], cls))
        for cls, (d1, d2, d3) in enumerate(CLASSES):
            w, s = b["w"][cls], b["s"][cls]
            b["ag"][cls][pos[d2], pos[d1]] = rows[:, s:s + w]

    def gather2(b):
        for cls, (d1, d2, d3) in enumerate(CLASSES):
            ag = b["ag"][cls]
            links.arrived(ag.at[0, 0:3], ("gather1", b["m"], cls))
            mine = ag.at[pos[d2]]
            for off in (1, 3):
                links.copy(mine, mine, along(d2, off)[1], ("gather2", b["m"], cls))

    def relay2(b):
        for cls, (d1, d2, d3) in enumerate(CLASSES):
            ag = b["ag"][cls]
            links.arrived(ag.at[0:2], ("gather2", b["m"], cls))
            for off, half in ((1, 0), (3, 2)):
                got = ag.at[along(d2, 4 - off)[0], half:half + 2]
                links.copy(got, got, along(d2, off)[1], ("relay2", b["m"], cls))

    def relayed(b, cls):
        links.arrived(b["ag"][cls].at[0], ("relay2", b["m"], cls))

    def pick(b, cls, off2):
        d1, d2, d3 = CLASSES[cls]
        w = b["w"][cls]
        block = along(d2, off2)[0]
        exp = iota((SIDE * CORES, 1), 0)
        exp = me - pos[d3] * STRIDE[d3] - core + (exp >> 1) * STRIDE[d3] + (exp & 1)
        rank = rank_of(routes[cls][block, b["m"]], exp.astype(F32))
        rank = jnp.concatenate([jnp.broadcast_to(rank[e:e + 1], (16, COLUMN)) for e in range(SIDE * CORES)], axis=0)
        slot = iota((COLUMN, 1), 0)
        mask = ((slot >> 2) & 3) == (iota((COLUMN, COLUMN), 1) >> 5)
        choice = ones_where(mask & (rank == (slot & 3).astype(F32)))
        got = dot(choice, b["ag"][cls][block].reshape(COLUMN, w)).astype(BF16)
        ps, pr = b["ps"][cls], b["pr"][cls]
        ps[block] = got.reshape(SIDE, CORES, 16, w)
        for off in (2, 1, 3, 0):
            there, dev = along(d3, off)
            first = dev - core
            for flip in (0, 1):
                there_core = core if flip == 0 else 1 - core
                if off == 0 and flip == 0:
                    pr[CORES * there + core, block] = ps[block, there, core]
                    continue
                links.copy(ps.at[block, there, there_core], pr.at[CORES * pos[d3] + core, block], first + there_core,
                           ("pick", b["m"], cls))

    def received(b):
        for cls in range(3):
            s, w = b["s"][cls], b["w"][cls]
            pr = b["pr"][cls]
            links.arrived(pr.at[0:7], ("pick", b["m"], cls))
            for c in range(CORES):
                rows = jnp.concatenate([pr[CORES * v + c].reshape(64, w) for v in range(SIDE)], axis=0)
                if cls:
                    rows = dot(perms[cls - 1], rows).astype(BF16)
                xbuf[:, c, :, s:s + w] = rows.reshape(SIDE, 64, w)

    def hidden(first, last):
        @pl.loop(first, last)
        def _(i):
            cols = pl.ds(pl.multiple_of(i * 256, 256), 256)
            x = xbuf[...].reshape(SLOTS, D)
            g = dot(x, vg[:, cols])
            u = dot(x, vu[:, cols])
            h = (g * (1.0 / (1.0 + jnp.exp(-g))) * u).astype(BF16)
            hbuf[:, :, :, cols] = h.reshape(SIDE, CORES, 64, 256)

    def lanes(b, cls, part):
        return (0, FIRST) if part == 0 else (FIRST, b["w"][cls])

    def align(b):
        for cls in (1, 2):
            for c in range(CORES):
                hperm[cls - 1, c] = dot(perms[cls + 1], hbuf[:, c].reshape(HALF, FF)).astype(BF16)

    def back1(b, part):
        for cls, (d1, d2, d3) in enumerate(CLASSES):
            s = b["s"][cls]
            lo, hi = lanes(b, cls, part)
            r1, y = b["r1"][cls], b["pr"][cls]
            for c in range(CORES):
                h = hperm[cls - 1, c] if cls else hbuf[:, c].reshape(HALF, FF)
                out = dot(h, vd[:, s + lo:s + hi]).astype(BF16).reshape(SIDE, SIDE, 16, hi - lo)
                for v in range(SIDE):
                    y[CORES * v + c, :, :, lo:hi] = out[v]
            for off in (2, 1, 3, 0):
                there, dev = along(d3, off)
                first = dev - core
                for flip in (0, 1):
                    there_core = core if flip == 0 else 1 - core
                    mine = y.at[CORES * there + there_core, :, :, lo:hi]
                    if off == 0 and flip == 0:
                        r1[there, core, :, :, lo:hi] = mine[...]
                        continue
                    links.copy(mine, r1.at[pos[d3], core, :, :, lo:hi], first + there_core,
                               ("back1", b["m"], cls), part, off)

    def back2(b, part):
        for cls, (d1, d2, d3) in enumerate(CLASSES):
            r1, r2 = b["r1"][cls], b["r2"][cls]
            lo, hi = lanes(b, cls, part)
            for off in (2, 0, 1, 3):
                chip = along(d3, (4 - off) % 4)[0]
                like = r1.at[0, :, :, :, lo:hi] if off else r1.at[0, 0, :, :, lo:hi]
                links.arrived(like, ("back1", b["m"], cls), part, off)
                for to in (2, 1, 3):
                    there, dev = along(d2, to)
                    links.copy(r1.at[chip, :, there, :, lo:hi], r2.at[pos[d2], chip, :, :, lo:hi], dev,
                               ("back2", b["m"], cls), part)
                r2[pos[d2], chip, :, :, lo:hi] = r1[chip, :, pos[d2], :, lo:hi]

    def weights(b, cls):
        d1, d2, d3 = CLASSES[cls]
        m = b["m"]
        route = routes[cls][pos[d2], m]
        gate = gates[cls][m]
        exp = iota((N_EXP, 1), 0).astype(F32)
        rank = rank_of(route, exp)
        value = jnp.zeros((N_EXP, COLUMN), F32)
        for j in range(TOP_K):
            value = jnp.where(route[j:j + 1] == exp, gate[j:j + 1], value)
        rank, value = rank.T.astype(BF16), value.T
        slot = iota((SLOTS, 1), 0)
        owner = pos[d1] * STRIDE[d1] + (slot >> 7) * STRIDE[d2] + ((slot >> 5) & 3) * STRIDE[d3] + ((slot >> 4) & 1)
        onehot = ones_where(iota((SLOTS, N_EXP), 1) == owner)
        col = iota((COLUMN, SLOTS), 1)
        keep = ((col >> 2) & 3) == (iota((COLUMN, SLOTS), 0) >> 5)
        keep = keep & (dot_nt(rank, onehot) == (col & 3).astype(F32))
        part1 = value.astype(BF16)
        rest = value - part1.astype(F32)
        part2 = rest.astype(BF16)
        part3 = (rest - part2.astype(F32)).astype(BF16)
        return jnp.concatenate(
            [jnp.where(keep, dot_nt(part, onehot), 0.0).astype(BF16) for part in (part3, part2, part1)], axis=0)

    def weigh(b):
        for cls in range(3):
            wts[cls] = weights(b, cls)

    def back3(b, part):
        for cls, (d1, d2, d3) in enumerate(CLASSES):
            lo, hi = lanes(b, cls, part)
            links.arrived(b["r2"][cls].at[0:3, :, :, :, lo:hi], ("back2", b["m"], cls), part)
            rows = b["r2"][cls][:, :, :, :, lo:hi].reshape(SLOTS, hi - lo)
            terms = dot(wts[cls], rows).reshape(3, COLUMN, hi - lo)
            sm, r3 = b["sm"][cls], b["r3"][cls]
            sm[:, :, lo:hi] = ((terms[0] + terms[1]) + terms[2]).reshape(SIDE, TOK, hi - lo)
            for off in (2, 1, 3):
                there, dev = along(d1, off)
                links.copy(sm.at[there, :, lo:hi], r3.at[pos[d1], :, lo:hi], dev, ("back3", b["m"], cls), part)
            r3[pos[d1], :, lo:hi] = sm[pos[d1], :, lo:hi]

    def finish(b, part, rows, out):
        for cls in range(3):
            s = b["s"][cls]
            lo, hi = lanes(b, cls, part)
            r3 = b["r3"][cls]
            links.arrived(r3.at[0:3, :, lo:hi], ("back3", b["m"], cls), part)
            total = (r3[0, :, lo:hi] + r3[1, :, lo:hi]) + (r3[2, :, lo:hi] + r3[3, :, lo:hi])
            out[:, s + lo:s + hi] = (rows[:, s + lo:s + hi].astype(F32) + total).astype(BF16)

    def drain(b, *names):
        for cls in range(3):
            likes = {"gather1": b["ag"][cls].at[0, 0:3], "gather2": b["ag"][cls].at[0:2], "relay2": b["ag"][cls].at[0],
                     "pick": b["pr"][cls].at[0:7], "back1": b["pr"][cls].at[0:7], "back2": b["r2"][cls].at[0:3],
                     "back3": b["r3"][cls].at[0:3]}
            for name in names:
                links.sent(likes[name], (name, b["m"], cls))

    a, b = batches
    write_meta()
    pl.semaphore_wait(barrier, len(peers))
    gather1(a, x_a)
    send_meta1()
    for i in range(4):
        proj_step(i)
    gather2(a)
    send_meta2()
    for i in range(4, n_wo):
        proj_step(i)
    u_b[...] = (h_b[...].astype(F32) + proj_acc[...].astype(BF16).astype(F32)).astype(BF16)
    gather1(b, u_b)
    for c in w_copies:
        c.start()
    wq_copy(0).start()
    wq_copy(1).start()
    for cls in range(3):
        pick(a, cls, 0)
    perms[0] = reorder(0, 1)
    perms[1] = reorder(0, 2)
    relay2(a)
    for cls in range(3):
        links.arrived(routes[cls].at[0:3], ("meta2", cls))
        pick(a, cls, 1)
        pick(a, cls, 3)
    gather2(b)
    for cls in range(3):
        relayed(a, cls)
        pick(a, cls, 2)
    for cls in range(3):
        pick(b, cls, 0)
    perms[2] = reorder(1, 0)
    perms[3] = reorder(2, 0)
    qkv_step(0)
    relay2(b)
    for cls in range(3):
        pick(b, cls, 1)
        pick(b, cls, 3)
    for c in w_copies:
        c.wait()
    received(a)
    hidden(0, 2)
    for cls in range(3):
        relayed(b, cls)
        pick(b, cls, 2)
    hidden(2, 3)
    align(a)
    back1(a, 0)
    back1(a, 1)
    qkv_step(1)
    qkv_step(2)
    received(b)
    hidden(0, 3)
    back2(a, 0)
    align(b)
    back1(b, 0)
    back2(a, 1)
    back1(b, 1)
    weigh(a)
    qkv_step(3)
    back3(a, 0)
    back2(b, 0)
    back3(a, 1)
    back2(b, 1)
    weigh(b)
    for i in range(4, n_wq):
        qkv_step(i)
    finish(a, 0, x_a, out_a)
    finish(a, 1, x_a, out_a)
    for cls in range(3):
        links.sent(meta[cls].at[0:3], ("meta1", cls))
        links.sent(routes[cls].at[0:3], ("meta2", cls))
    drain(a, "gather1", "gather2", "relay2", "pick", "back1", "back2", "back3")
    drain(b, "gather1", "gather2", "relay2", "pick", "back1")
    back3(b, 0)
    back3(b, 1)
    finish(b, 0, u_b, out_b)
    drain(b, "back2")
    finish(b, 1, u_b, out_b)
    drain(b, "back3")


def deliver(*refs):
    n = (len(refs) - 1) // 2
    ops = [pltpu.make_async_copy(refs[i], refs[n + i], refs[-1].at[i]) for i in range(n)]
    for op in ops:
        op.start()
    for op in ops:
        op.wait()


def solution(mesh):
    def local_step(x_a, route_a, gate_a, h_b, attn_b, route_b, gate_b, w_qkv, w_o, w_gate, w_up, w_down):
        vmem = pl.BlockSpec(memory_space=pltpu.VMEM)
        hbm = pl.BlockSpec(memory_space=pl.ANY)
        scratch = []
        for m in range(2):
            for shape, dtype in (
                (lambda w: (SIDE, SIDE, TOK, w), BF16),
                (lambda w: (SIDE, SIDE, CORES, 16, w), BF16),
                (lambda w: (SIDE * CORES, SIDE, 16, w), BF16),
                (lambda w: (SIDE, CORES, SIDE, 16, w), BF16),
                (lambda w: (SIDE, SIDE, CORES, 16, w), BF16),
                (lambda w: (SIDE, TOK, w), F32),
                (lambda w: (SIDE, TOK, w), F32),
            ):
                scratch += [pltpu.VMEM(shape(w), dtype) for w in WIDTHS[m]]
        scratch += [pltpu.VMEM((SIDE, 2, TOP_K, COLUMN), F32)] * 3
        scratch += [pltpu.VMEM((SIDE, 2, TOP_K, COLUMN), F32)] * 3
        scratch += [pltpu.VMEM((2, TOP_K, COLUMN), F32)] * 3
        scratch += [
            pltpu.VMEM((SIDE, CORES, 64, D), BF16),
            pltpu.VMEM((SIDE, CORES, 64, FF), BF16),
            pltpu.VMEM((2, CORES, HALF, FF), BF16),
            pltpu.VMEM((3, 3 * COLUMN, SLOTS), BF16),
            pltpu.VMEM((4, HALF, HALF), BF16),
            pltpu.VMEM((TOK, D), F32),
            pltpu.VMEM((TOK, QKV), F32),
            pltpu.VMEM((TOK, D), BF16),
            pltpu.VMEM((D, FF), BF16),
            pltpu.VMEM((D, FF), BF16),
            pltpu.VMEM((FF, D), BF16),
            pltpu.VMEM((2, WO_CHUNK, D), BF16),
            pltpu.VMEM((2, WQ_CHUNK, QKV), BF16),
            pltpu.SemaphoreType.DMA((N_PHASES,)),
            pltpu.SemaphoreType.DMA((N_GROUPS,)),
            pltpu.SemaphoreType.DMA((3,)),
            pltpu.SemaphoreType.DMA((2,)),
            pltpu.SemaphoreType.DMA((2,)),
        ]
        outs = tuple(jax.ShapeDtypeStruct((TOK, n), BF16) for n in (D, D, QKV))
        results = pl.pallas_call(
            kernel,
            out_shape=outs,
            in_specs=[vmem] * 7 + [hbm] * 5,
            out_specs=(vmem,) * 3,
            scratch_shapes=scratch,
            name="moe_pair",
            compiler_params=pltpu.CompilerParams(
                collective_id=0, has_side_effects=True, vmem_limit_bytes=64 * 2**20 - 2**16),
        )(x_a, h_b, attn_b, route_a.T, route_b.T, gate_a.T, gate_b.T, w_qkv, w_o, w_gate, w_up, w_down)
        return pl.pallas_call(
            deliver,
            out_shape=outs,
            in_specs=[hbm] * 3,
            out_specs=(vmem,) * 3,
            scratch_shapes=[pltpu.SemaphoreType.DMA((3,))],
            name="deliver",
        )(*results)

    row_spec = P(("dp", "ep"), None)
    full_spec = P(None, None)
    expert_spec = P("ep", None, None)
    return jax.shard_map(
        local_step,
        mesh=mesh,
        in_specs=(row_spec,) * 7 + (full_spec, full_spec) + (expert_spec,) * 3,
        out_specs=(row_spec, row_spec, row_spec),
        check_vma=False,
    )
```
